32 devices in a mesh: freq: 8 (over z, x), kgrp: 4 (over y, core).
Axes of the slice: x: 2, y: 2, z: 4, core: 2. Of those that a mesh axis runs over, the one named last changes fastest.
Arguments:
- hamiltonian: float32 [256, 64, 128], P(('freq', 'kgrp')), may hold values from -1 to 1, as said below
- self_energy: float32 [16, 64, 128], P('freq'), may hold values from -0.8 to 0.3, as said below
- guess_factor: float32 [16, 64, 128], P('freq'), may hold values from -0.05 to 1.25
- weights: int32 [256], replicated, may hold values from 1 to 48
- counts: int32 [16], replicated, may hold values from 1 to 3, as said below
Outputs:
- local_green: float32 [4096, 32], P(('freq', 'kgrp'))
The draws below stay inside these ranges and needn't reach their ends.
Inputs may be any that keep to these rules, and one draw needn't show every extreme that they name: `hamiltonian`: each k-point's matrix is Hermitian: the left half symmetric, the right half antisymmetric. `self_energy`: the diagonal of the right half lies between -0.8 and -0.4. `counts`: the number of Newton-Schulz steps taken at each frequency.
All inputs are finite; a program needn't handle non-finite values.
Results may differ from the reference program's by a relative error of at most 0.0001.
Values sent between devices are 32-bit elements.
A program may use at most 64 MiB of HBM per device.

```python
import math
import jax
import jax.numpy as jnp
from jax import lax

NORB = 64
MAXIT = 3
FREQ = 16
KPTS = 256


def noise_draw(key, shape, spread):
    return jax.random.truncated_normal(key, -4.0, 4.0, shape, jnp.float32) * spread


def draw_hamiltonian(key, part):
    first_key, second_key, third_key = jax.random.split(key, 3)
    identity = jnp.eye(NORB, dtype=jnp.float32)
    left_noise = noise_draw(first_key, (KPTS, NORB, NORB), 0.018)
    right_noise = noise_draw(second_key, (KPTS, NORB, NORB), 0.018)
    symmetric = (left_noise + jnp.swapaxes(left_noise, 1, 2)) * 0.70710678 * (1.0 - identity)
    skewed = (right_noise - jnp.swapaxes(right_noise, 1, 2)) * 0.70710678
    levels = jax.random.uniform(third_key, (KPTS, NORB), jnp.float32, -1.0, 1.0)
    real_part = symmetric + levels[:, :, None] * identity
    return jnp.concatenate([real_part, skewed], -1).astype(jnp.float32)


def draw_self_energy(key, part):
    first_key, second_key, third_key, fourth_key = jax.random.split(key, 4)
    identity = jnp.eye(NORB, dtype=jnp.float32)
    real_off = noise_draw(first_key, (FREQ, NORB, NORB), 0.012) * (1.0 - identity)
    imag_off = noise_draw(second_key, (FREQ, NORB, NORB), 0.012) * (1.0 - identity)
    real_diag = jax.random.uniform(third_key, (FREQ, NORB), jnp.float32, -0.3, 0.3)
    damping = jax.random.uniform(fourth_key, (FREQ, NORB), jnp.float32, -0.8, -0.4)
    real_part = real_off + real_diag[:, :, None] * identity
    imag_part = imag_off + damping[:, :, None] * identity
    return jnp.concatenate([real_part, imag_part], -1).astype(jnp.float32)


def draw_guess_factor(key, part):
    first_key, second_key, third_key = jax.random.split(key, 3)
    identity = jnp.eye(NORB, dtype=jnp.float32)
    real_off = noise_draw(first_key, (FREQ, NORB, NORB), 0.01) * (1.0 - identity)
    imag_part = noise_draw(second_key, (FREQ, NORB, NORB), 0.01)
    scales = jax.random.uniform(third_key, (FREQ, NORB), jnp.float32, 0.75, 1.25)
    real_part = real_off + scales[:, :, None] * identity
    return jnp.concatenate([real_part, imag_part], -1).astype(jnp.float32)


def draw_counts(key, part):
    positions = jnp.arange(FREQ, dtype=jnp.int32)
    extra = jax.random.randint(key, (FREQ,), 0, 4)
    lowest = (8 * positions < FREQ).astype(jnp.int32)
    bumped = ((extra == 0) & (positions < FREQ - 1)).astype(jnp.int32)
    return jnp.minimum(MAXIT, 1 + 2 * lowest + bumped).astype(jnp.int32)


def set_ends(drawn, stream_key, smallest, high):
    longest = drawn.shape.index(max(drawn.shape))
    spots = []
    for shift in (0, 1):
        where = [jax.random.randint(jax.random.fold_in(stream_key, axis), (), 0, length) for axis, length in enumerate(drawn.shape)]
        where[longest] = (where[longest] + shift) % drawn.shape[longest]
        spots.append(tuple(where))
    return drawn.at[spots[0]].set(smallest).at[spots[1]].set(high)


def setup_inputs(seed: int = 0) -> dict:
    keys = jax.random.split(jax.random.key(seed), 6)
    hamiltonian = draw_hamiltonian(jax.random.fold_in(keys[5], 71), 0)
    self_energy = draw_self_energy(jax.random.fold_in(keys[5], 71), 0)
    guess_factor = draw_guess_factor(jax.random.fold_in(keys[5], 71), 0)
    weights = set_ends(jax.random.randint(keys[3], (KPTS,), 1, 49), jax.random.fold_in(keys[3], 1), 1, 48).astype(jnp.int32)
    counts = draw_counts(jax.random.fold_in(keys[5], 71), 0)
    return dict(hamiltonian=hamiltonian, self_energy=self_energy, guess_factor=guess_factor, weights=weights, counts=counts)


chem_potential = 0.2


def blockify(right_side):
    order = right_side.shape[-1] // 2
    real_part = right_side[..., :order]
    imag_part = right_side[..., order:]
    upper_row = jnp.concatenate([real_part, imag_part], -1)
    lower_row = jnp.concatenate([-imag_part, real_part], -1)
    return jnp.concatenate([upper_row, lower_row], -2)


def complex_product(left_side, right_side):
    return jnp.einsum('...ij,...jl->...il', left_side, blockify(right_side), precision=lax.Precision.HIGHEST)


def build_matrix(kpoint_rows, sigma_rows, matsubara):
    orbitals = kpoint_rows.shape[1]
    identity = jnp.eye(orbitals, dtype=jnp.float32)
    real_shift = jnp.broadcast_to(chem_potential * identity, matsubara.shape + identity.shape)
    imag_shift = matsubara[:, None, None] * identity
    diagonal_shift = jnp.concatenate([real_shift, imag_shift], -1)
    return diagonal_shift[:, None] - kpoint_rows[None] - sigma_rows[:, None]


def start_guess(matrix, factor_rows):
    orbitals = matrix.shape[-2]
    diag_real = jnp.diagonal(matrix[..., :orbitals], axis1=-2, axis2=-1)
    diag_imag = jnp.diagonal(matrix[..., orbitals:], axis1=-2, axis2=-1)
    modulus = diag_real * diag_real + diag_imag * diag_imag
    recip_real = (diag_real / modulus)[..., None]
    recip_imag = (-diag_imag / modulus)[..., None]
    factor_real = factor_rows[..., :orbitals]
    factor_imag = factor_rows[..., orbitals:]
    guess_real = recip_real * factor_real - recip_imag * factor_imag
    guess_imag = recip_real * factor_imag + recip_imag * factor_real
    return jnp.concatenate([guess_real, guess_imag], -1)


def reference(hamiltonian, self_energy, guess_factor, weights, counts):
    orbitals = hamiltonian.shape[1]
    factors = weights.astype(jnp.float32)
    weight_total = jnp.sum(factors)
    identity = jnp.eye(orbitals, dtype=jnp.float32)
    doubled = jnp.concatenate([2.0 * identity, jnp.zeros_like(identity)], -1)

    def one_frequency(inputs):
        sigma_row, factor_row, step_count, freq_id = inputs
        matsubara = (2 * freq_id + 1).astype(jnp.float32)[None] * (math.pi / (2 * FREQ))
        matrix = build_matrix(hamiltonian, sigma_row[None], matsubara)
        initial = start_guess(matrix, factor_row[None, None])

        def newton_step(sweep, current):
            return complex_product(current, doubled - complex_product(matrix, current))

        final = lax.fori_loop(0, step_count, newton_step, initial)
        summed = jnp.einsum('k,fkij->fij', factors, final, precision=lax.Precision.HIGHEST)
        return summed[0] / weight_total

    greens = lax.map(one_frequency, (self_energy, guess_factor, counts, jnp.arange(FREQ, dtype=jnp.int32)))
    arranged = greens.reshape(FREQ, orbitals, 2, orbitals).transpose(1, 3, 2, 0)
    return arranged.reshape(orbitals * orbitals, 2 * FREQ)
```

```python
import functools
import math

import jax
import jax.numpy as jnp
from jax import lax
from jax.experimental import pallas as pl
from jax.experimental.pallas import tpu as pltpu
from jax.sharding import PartitionSpec as P

chem_potential = 0.2
MESH = pl.DeviceIdType.MESH
GRANT = 32 * 1024 * 1024
VMEM = pl.BlockSpec(memory_space=pltpu.VMEM)
SMEM = pl.BlockSpec(memory_space=pltpu.SMEM)
ANY = pl.BlockSpec(memory_space=pl.ANY)


def split(value):
    high = value.astype(jnp.bfloat16).astype(jnp.float32)
    return high, value - high


def left_operand(value, half, left):
    high, low = split(value)
    turned_high, turned_low = split(pltpu.roll(value, half, 1))
    top = jnp.where(left, high, turned_low)
    bottom = jnp.where(left, turned_high, low)
    return jnp.concatenate([top, bottom], 0).astype(jnp.bfloat16)


def right_operand(value):
    high, low = split(value)
    row = jnp.concatenate([high, low], 1).astype(jnp.bfloat16)
    return jnp.concatenate([row, row], 0)


def fold(product, orbitals, sign):
    width = 2 * orbitals
    both = product[:, :width] + product[:, width:]
    return both[:orbitals] + sign * pltpu.roll(both[orbitals:], orbitals, 1)


def masks(shape):
    orbitals = shape[0]
    row = lax.broadcasted_iota(jnp.int32, shape, 0)
    lane = lax.broadcasted_iota(jnp.int32, shape, 1)
    left = lane < orbitals
    sign = jnp.where(left, -1.0, 1.0)
    eye_real = (lane == row).astype(jnp.float32)
    eye_imag = (lane == row + orbitals).astype(jnp.float32)
    return left, sign, eye_real, eye_imag


def shifted(freq, freq_total, eye_real, eye_imag, sigma):
    matsubara = (2 * freq + 1).astype(jnp.float32) * (math.pi / (2 * freq_total))
    return (chem_potential * eye_real + matsubara * eye_imag) - sigma


def steps_kernel(counts, weights, h_ref, sigma_ref, guess_ref, x_ref, factor_ref, m_left, h_diag):
    k_local, orbitals, width = h_ref.shape
    freq_total = sigma_ref.shape[0]
    shape = (orbitals, width)
    left, sign, eye_real, eye_imag = masks(shape)
    device = lax.axis_index("freq") * lax.axis_size("kgrp") + lax.axis_index("kgrp")

    def add_weight(index, total):
        return total + weights[index]

    weight_total = lax.fori_loop(
        0, weights.shape[0], add_weight, jnp.int32(0), unroll=8
    ).astype(jnp.float32)
    for k in range(k_local):
        weight = weights[device * k_local + k].astype(jnp.float32)
        factor_ref[k : k + 1, :] = jnp.full((1, width), weight) / weight_total

    def diagonal(value):
        real = jnp.sum(value * eye_real, axis=1, keepdims=True)
        imag = jnp.sum(value * eye_imag, axis=1, keepdims=True)
        return jnp.broadcast_to(real, shape), jnp.broadcast_to(imag, shape)

    for k in range(k_local):
        h_diag[0, k], h_diag[1, k] = diagonal(h_ref[k])

    def one_frequency(freq, carry):
        base = shifted(freq, freq_total, eye_real, eye_imag, sigma_ref[freq])
        base_real, base_imag = diagonal(base)
        guess = guess_ref[freq]
        turned = sign * pltpu.roll(guess, orbitals, 1)
        for k in range(k_local):
            real = base_real - h_diag[0, k]
            imag = base_imag - h_diag[1, k]
            inverse = 1.0 / (real * real + imag * imag)
            x_ref[freq, k] = (real * inverse) * guess - (imag * inverse) * turned

        @pl.when(counts[freq] > 1)
        def _():
            for k in range(k_local):
                m_left[k] = left_operand(base - h_ref[k], orbitals, left)

            def newton_step(sweep, inner):
                products = [
                    jnp.dot(
                        m_left[k],
                        right_operand(x_ref[freq, k]),
                        preferred_element_type=jnp.float32,
                    )
                    for k in range(k_local)
                ]
                products = [
                    jnp.dot(
                        left_operand(x_ref[freq, k], orbitals, left),
                        right_operand(eye_real - fold(products[k], orbitals, sign)),
                        preferred_element_type=jnp.float32,
                    )
                    for k in range(k_local)
                ]
                for k in range(k_local):
                    x_ref[freq, k] = x_ref[freq, k] + fold(products[k], orbitals, sign)
                return inner

            lax.fori_loop(0, counts[freq] - 1, newton_step, 0)

        return carry

    lax.fori_loop(0, freq_total, one_frequency, 0)


def early_steps(counts, weights, hamiltonian, sigma, guess):
    k_local, orbitals, width = hamiltonian.shape
    freq_total = sigma.shape[0]
    return pl.pallas_call(
        steps_kernel,
        out_shape=(
            jax.ShapeDtypeStruct((freq_total, k_local, orbitals, width), jnp.float32),
            jax.ShapeDtypeStruct((k_local, width), jnp.float32),
        ),
        in_specs=[SMEM, SMEM, VMEM, VMEM, VMEM],
        out_specs=(VMEM, VMEM),
        scratch_shapes=[
            pltpu.VMEM((k_local, width, width), jnp.bfloat16),
            pltpu.VMEM((2, k_local, orbitals, width), jnp.float32),
        ],
        compiler_params=pltpu.CompilerParams(vmem_limit_bytes=GRANT),
        name="early_steps",
    )(counts, weights, hamiltonian, sigma, guess)


def last_step(freq, freq_total, factor_ref, h_ref, sigma_ref, x_ref, last_left, last_right):
    k_local, orbitals, width = h_ref.shape
    left, sign, eye_real, eye_imag = masks((orbitals, width))
    base = shifted(freq, freq_total, eye_real, eye_imag, sigma_ref[freq])
    products = [
        jnp.dot(
            left_operand(base - h_ref[k], orbitals, left),
            right_operand(x_ref[freq, k]),
            preferred_element_type=jnp.float32,
        )
        for k in range(k_local)
    ]
    total = jnp.zeros((orbitals, width), jnp.float32)
    for k in range(k_local):
        weighted = x_ref[freq, k] * factor_ref[k : k + 1, :]
        last_left[:, k * width : (k + 1) * width] = left_operand(weighted, orbitals, left)
        total = total + weighted
    for k in range(k_local):
        missing = eye_real - fold(products[k], orbitals, sign)
        last_right[k * width : (k + 1) * width, :] = right_operand(missing)
    product = jnp.dot(last_left[...], last_right[...], preferred_element_type=jnp.float32)
    return total + fold(product, orbitals, sign)


def last_scratch(k_local, width):
    return [
        pltpu.VMEM((width, k_local * width), jnp.bfloat16),
        pltpu.VMEM((k_local * width, 2 * width), jnp.bfloat16),
    ]


def sum_kernel(factor_ref, h_ref, sigma_ref, x_ref, out_ref, last_left, last_right):
    freq_total = sigma_ref.shape[0]

    def one_frequency(freq, carry):
        out_ref[freq] = last_step(
            freq, freq_total, factor_ref, h_ref, sigma_ref, x_ref, last_left, last_right
        )
        return carry

    lax.fori_loop(0, freq_total, one_frequency, 0)


def local_sum(factors, hamiltonian, sigma, current):
    k_local, orbitals, width = hamiltonian.shape
    return pl.pallas_call(
        sum_kernel,
        out_shape=jax.ShapeDtypeStruct(sigma.shape, jnp.float32),
        in_specs=[VMEM] * 4,
        out_specs=VMEM,
        scratch_shapes=last_scratch(k_local, width),
        name="local_sum",
    )(factors, hamiltonian, sigma, current)


def gather_kernel(h_hbm, sigma_hbm, guess_hbm, h_out, sg_out, local, mate_sem, pair_sem, pass_sem, col_sem):
    pieces, k_local = h_out.shape[0], h_out.shape[1]
    column = sg_out.shape[0]
    freq_devs = 2 * column
    me = lax.axis_index("freq")
    group = lax.axis_index("kgrp")
    parity = lax.rem(group, 2)
    place = me // 2
    pair = me + 1 - 2 * lax.rem(me, 2)
    mate = group + 1 - 2 * parity
    barrier = pltpu.get_barrier_semaphore()
    for shift in range(1, column):
        pl.semaphore_signal(
            barrier, inc=1, device_id=(lax.rem(me + 2 * shift, freq_devs), group), device_id_type=MESH
        )
    pl.semaphore_signal(barrier, inc=1, device_id=(pair, group), device_id_type=MESH)
    pl.semaphore_signal(barrier, inc=1, device_id=(me, mate), device_id_type=MESH)
    loads = [
        pltpu.make_async_copy(h_hbm, h_out.at[0], local.at[0]),
        pltpu.make_async_copy(sigma_hbm.at[parity], sg_out.at[place, 0], local.at[1]),
        pltpu.make_async_copy(guess_hbm.at[parity], sg_out.at[place, 1], local.at[2]),
    ]
    for load in loads:
        load.start()

    def remote(src, dst, sems, slot, freq_to, group_to):
        return pltpu.make_async_remote_copy(
            src_ref=src,
            dst_ref=dst,
            send_sem=sems.at[0, slot],
            recv_sem=sems.at[1, slot],
            device_id=(freq_to, group_to),
            device_id_type=MESH,
        )

    chunks = pair_sem.shape[1]
    step = k_local // chunks
    own = sg_out.at[place]
    columns = [
        remote(own, own, col_sem, shift, lax.rem(me + 2 * shift, freq_devs), group)
        for shift in range(1, column)
    ]
    across = [
        remote(
            h_out.at[0, pl.ds(c * step, step)], h_out.at[2, pl.ds(c * step, step)], pair_sem, c, pair, group
        )
        for c in range(chunks)
    ]
    passes = [
        remote(
            h_out.at[2, pl.ds(c * step, step)], h_out.at[3, pl.ds(c * step, step)], pass_sem, c, me, mate
        )
        for c in range(chunks)
    ]
    beside = remote(h_out.at[0], h_out.at[1], mate_sem, 0, me, mate)
    for load in loads:
        load.wait()
    pl.semaphore_wait(barrier, column + 1)
    for copy in columns + across + [beside]:
        copy.start()
    for c in range(chunks):
        across[c].wait_recv()
        passes[c].start()
    beside.wait()
    for copy in columns:
        copy.wait()
    for copy in passes:
        copy.wait()
    for copy in across:
        copy.wait_send()


def gather(hamiltonian, self_energy, guess_factor, column):
    k_local, orbitals, width = hamiltonian.shape
    chunks = 4 if k_local % 4 == 0 else 1
    pairs = pltpu.SemaphoreType.DMA((2, chunks))
    return pl.pallas_call(
        gather_kernel,
        out_shape=(
            jax.ShapeDtypeStruct((4, k_local, orbitals, width), jnp.float32),
            jax.ShapeDtypeStruct((column, 2, orbitals, width), jnp.float32),
        ),
        in_specs=[ANY] * 3,
        out_specs=(VMEM, VMEM),
        scratch_shapes=[
            pltpu.SemaphoreType.DMA((3,)),
            pltpu.SemaphoreType.DMA((2, 1)),
            pairs,
            pairs,
            pltpu.SemaphoreType.DMA((2, column)),
        ],
        compiler_params=pltpu.CompilerParams(collective_id=0, has_side_effects=True, vmem_limit_bytes=GRANT),
        name="gather",
    )(hamiltonian, self_energy, guess_factor)


def halves(value):
    high = value.astype(jnp.bfloat16)
    return high, (value - high.astype(jnp.float32)).astype(jnp.bfloat16)


def side(value):
    return jnp.concatenate(halves(value), 1)


def block(value, turned):
    top = side(value)
    bottom = side(turned)
    return jnp.concatenate([top, bottom, top, bottom], 0)


def joined(product):
    width = product.shape[1] // 2
    return product[:, :width] + product[:, width:]


def dot(left_side, right_side):
    return jnp.dot(left_side, right_side, preferred_element_type=jnp.float32)


def newton_kernel(
    h_ref,
    sg_ref,
    weights_hbm,
    counts_hbm,
    out_ref,
    weights,
    counts,
    load_sem,
    g_side,
    g_shift,
    rows,
    shift_rows,
    columns,
    f_ref,
    left_ref,
    right_ref,
    work,
    total_ref,
):
    slots, k_local, orbitals, width = h_ref.shape
    column = sg_ref.shape[0]
    freq_total = counts_hbm.shape[0]
    shape = (orbitals, width)
    me = lax.axis_index("freq")
    group = lax.axis_index("kgrp")
    group_devs = lax.axis_size("kgrp")
    parity = lax.rem(group, 2)
    branch = lax.rem(me, 2)
    loads = [
        pltpu.make_async_copy(weights_hbm, weights, load_sem.at[0]),
        pltpu.make_async_copy(counts_hbm, counts, load_sem.at[1]),
    ]
    for load in loads:
        load.start()
    left, sign, eye_real, eye_imag = masks(shape)

    def turn(value):
        return sign * pltpu.roll(value, orbitals, 1)

    def frequency(index):
        return 2 * (2 * index + branch) + parity

    def diagonal_rows(value, rolled):
        real = jnp.sum(eye_real * value + eye_imag * rolled, axis=0, keepdims=True)
        return real

    for index in range(column):
        base = shifted(frequency(index), freq_total, eye_real, eye_imag, sg_ref[index, 0])
        guess = sg_ref[index, 1]
        g_side[index * orbitals : (index + 1) * orbitals, :] = side(guess)
        rolled = pltpu.roll(base, orbitals, 1)
        shift_rows[2 * index : 2 * index + 1, :] = diagonal_rows(base, rolled)
        shift_rows[2 * index + 1 : 2 * index + 2, :] = diagonal_rows(rolled, base)
        g_shift[index] = joined(
            dot(g_side[index * orbitals : (index + 1) * orbitals, :], block(base, sign * rolled))
        )
    for load in loads:
        load.wait()

    tile = (k_local, width)
    k_row = lax.broadcasted_iota(jnp.int32, tile, 0)
    tile_left = lax.broadcasted_iota(jnp.int32, tile, 1) < orbitals

    def first(slot, carry):
        owner_freq = jnp.where(slot < 2, me, me + 1 - 2 * branch)
        owner_group = jnp.where(lax.rem(slot, 2) == 0, group, group + 1 - 2 * parity)
        k_first = (owner_freq * group_devs + owner_group) * k_local
        weight = jnp.zeros(tile, jnp.float32)
        for j in range(k_local):
            position = k_first + j
            value = weights[position // width, lax.rem(position, width)].astype(jnp.float32)
            weight = jnp.where(k_row == j, value, weight)
        h_diag = []
        blocks = []
        for j in range(k_local):
            value = h_ref[slot, j]
            rolled = pltpu.roll(value, orbitals, 1)
            h_diag.append(diagonal_rows(value, rolled))
            blocks.append(block(value, sign * rolled))
        h_diag = jnp.concatenate(h_diag, 0)
        scales = []
        for index in range(column):
            real = shift_rows[2 * index : 2 * index + 1, :] - h_diag
            imag = shift_rows[2 * index + 1 : 2 * index + 2, :]
            inverse = 1.0 / (real * real + imag * imag)
            d_real = real * inverse
            d_imag = -imag * inverse
            rows[index, slot, 0] = d_real
            rows[index, slot, 1] = jnp.where(tile_left, -d_imag, d_imag)
            columns[index, slot] = jnp.transpose(weight * jnp.where(tile_left, d_real, d_imag))
        for j in range(k_local):
            product = joined(dot(g_side[...], blocks[j]))
            for index in range(column):
                q = g_shift[index] - product[index * orbitals : (index + 1) * orbitals, :]
                turned = pltpu.roll(q, orbitals, 1)
                f_ref[index, slot, j] = (
                    eye_real - q * rows[index, slot, 0, j : j + 1, :] - turned * rows[index, slot, 1, j : j + 1, :]
                )
        return carry

    lax.fori_loop(0, slots, first, 0)

    def scaled(index, slot, j, value):
        d_real = jnp.broadcast_to(columns[index, slot, 0:orbitals, j : j + 1], shape)
        d_imag = jnp.broadcast_to(columns[index, slot, orbitals:width, j : j + 1], shape)
        return d_real * value + d_imag * turn(value)

    def finish(index, slot, outer, inner):
        terms = jnp.zeros(shape, jnp.float32)
        for j in range(k_local):
            term = scaled(index, slot, j, outer(j))
            terms = terms + term
            left_ref[:, 2 * j * width : 2 * (j + 1) * width] = side(term)
            value = inner(j)
            right_ref[2 * j * width : 2 * (j + 1) * width, :] = block(value, turn(value))
        total_ref[...] += terms + joined(dot(left_ref[...], right_ref[...]))

    def one_frequency(index, carry):
        count = counts[frequency(index)]
        total_ref[...] = jnp.zeros(shape, jnp.float32)

        @pl.when(count == 1)
        def _():
            def sweep(slot, inner):
                terms = jnp.zeros(shape, jnp.float32)
                for j in range(k_local):
                    terms = terms + scaled(index, slot, j, eye_real + f_ref[index, slot, j])
                total_ref[...] += terms
                return inner

            lax.fori_loop(0, slots, sweep, 0)

        @pl.when(count > 1)
        def _():
            def sweep(slot, inner):
                for j in range(k_local):
                    value = f_ref[index, slot, j]
                    work[0, j] = joined(dot(side(value), block(value, turn(value))))

                @pl.when(count == 2)
                def _():
                    finish(index, slot, lambda j: eye_real + f_ref[index, slot, j], lambda j: work[0, j])

                @pl.when(count > 2)
                def _():
                    for j in range(k_local):
                        value = f_ref[index, slot, j]
                        square = work[0, j]
                        both = jnp.concatenate([side(value), side(square)], 0)
                        product = joined(dot(both, block(square, turn(square))))
                        work[1, j] = eye_real + value + square + product[:orbitals]
                        work[2, j] = product[orbitals:]
                    finish(index, slot, lambda j: work[1, j], lambda j: work[2, j])

                return inner

            lax.fori_loop(0, slots, sweep, 0)

        guess = sg_ref[index, 1]
        green = joined(dot(side(total_ref[...]), block(guess, turn(guess))))
        out_ref[pl.ds(index, orbitals, stride=column), :] = green
        return carry

    lax.fori_loop(0, column, one_frequency, 0)


def newton(hamiltonians, sigma_guess, weights, counts):
    slots, k_local, orbitals, width = hamiltonians.shape
    column = sigma_guess.shape[0]
    return pl.pallas_call(
        newton_kernel,
        out_shape=jax.ShapeDtypeStruct((column * orbitals, width), jnp.float32),
        in_specs=[VMEM, VMEM, ANY, ANY],
        out_specs=VMEM,
        scratch_shapes=[
            pltpu.SMEM(weights.shape, jnp.int32),
            pltpu.SMEM(counts.shape, jnp.int32),
            pltpu.SemaphoreType.DMA((2,)),
            pltpu.VMEM((column * orbitals, 2 * width), jnp.bfloat16),
            pltpu.VMEM((column, orbitals, width), jnp.float32),
            pltpu.VMEM((column, slots, 2, k_local, width), jnp.float32),
            pltpu.VMEM((2 * column, width), jnp.float32),
            pltpu.VMEM((column, slots, width, k_local), jnp.float32),
            pltpu.VMEM((column, slots, k_local, orbitals, width), jnp.float32),
            pltpu.VMEM((orbitals, 2 * k_local * width), jnp.bfloat16),
            pltpu.VMEM((2 * k_local * width, 2 * width), jnp.bfloat16),
            pltpu.VMEM((3, k_local, orbitals, width), jnp.float32),
            pltpu.VMEM((orbitals, width), jnp.float32),
        ],
        compiler_params=pltpu.CompilerParams(vmem_limit_bytes=GRANT),
        name="newton",
    )(hamiltonians, sigma_guess, weights, counts)


def scatter_kernel(part, weights_hbm, out_ref, weights, landed, staged, load_sem, send, recv):
    freq_devs = lax.axis_size("freq")
    group_devs = lax.axis_size("kgrp")
    column = freq_devs // 2
    tile, width = landed.shape[2:]
    orbitals = width // 2
    me = lax.axis_index("freq")
    group = lax.axis_index("kgrp")
    others = [(a, b) for a in range(freq_devs) for b in range(group_devs) if a + b > 0]
    barrier = pltpu.get_barrier_semaphore()

    def place(step):
        return lax.rem(me + step[0], freq_devs), lax.rem(group + step[1], group_devs)

    for step in others:
        pl.semaphore_signal(barrier, inc=1, device_id=place(step), device_id_type=MESH)
    load = pltpu.make_async_copy(weights_hbm, weights, load_sem.at[0])
    load.start()

    def spread(index):
        freq_to, group_to = place(others[index])
        return pltpu.make_async_remote_copy(
            src_ref=part.at[pl.ds((freq_to * group_devs + group_to) * tile, tile)],
            dst_ref=landed.at[me, group],
            send_sem=send.at[index],
            recv_sem=recv.at[index],
            device_id=(freq_to, group_to),
            device_id_type=MESH,
        )

    pl.semaphore_wait(barrier, len(others))
    for index in range(len(others)):
        spread(index).start()
    landed[me, group] = part[pl.ds((me * group_devs + group) * tile, tile), :]
    load.wait()
    total = jnp.sum(weights[...].astype(jnp.float32), axis=0, keepdims=True)
    scale = 1.0 / jnp.broadcast_to(jnp.sum(total, axis=1, keepdims=True), (tile, width))
    for index in range(len(others)):
        spread(index).wait_recv()
    left = lax.broadcasted_iota(jnp.int32, (tile, width), 1) < orbitals
    freq_total = 4 * column
    for branch in range(2):
        for parity in range(2):
            total = None
            for place_at in range(column):
                for high in range(group_devs // 2):
                    term = landed[2 * place_at + branch, 2 * high + parity]
                    total = term if total is None else total + term
            total = total * scale
            swapped = pltpu.roll(total, tile // 2, 0)
            turned = pltpu.roll(total, orbitals, 1)
            turned_swapped = pltpu.roll(turned, tile // 2, 0)
            real = jnp.where(left, total, turned_swapped)
            imag = jnp.where(left, turned, swapped)
            first = 2 * branch + parity
            staged[pl.ds(first, column, stride=4), :] = real[:column]
            staged[pl.ds(freq_total + first, column, stride=4), :] = imag[:column]
    out_ref[...] = jnp.transpose(staged[...])
    for index in range(len(others)):
        spread(index).wait_send()


def scatter(part, weights, freq_devs, group_devs):
    width = part.shape[1]
    tile = part.shape[0] // (freq_devs * group_devs)
    column = freq_devs // 2
    peers = freq_devs * group_devs - 1
    return pl.pallas_call(
        scatter_kernel,
        out_shape=jax.ShapeDtypeStruct((width, 8 * column), jnp.float32),
        in_specs=[VMEM, ANY],
        out_specs=VMEM,
        scratch_shapes=[
            pltpu.VMEM(weights.shape, jnp.int32),
            pltpu.VMEM((freq_devs, group_devs, tile, width), jnp.float32),
            pltpu.VMEM((8 * column, width), jnp.float32),
            pltpu.SemaphoreType.DMA((1,)),
            pltpu.SemaphoreType.DMA((peers,)),
            pltpu.SemaphoreType.DMA((peers,)),
        ],
        compiler_params=pltpu.CompilerParams(collective_id=1, has_side_effects=True, vmem_limit_bytes=GRANT),
        name="scatter",
    )(part, weights)


def per_device(hamiltonian, self_energy, guess_factor, weights, counts):
    k_local, orbitals, width = hamiltonian.shape
    per_freq = self_energy.shape[0]
    freq_devs = lax.axis_size("freq")
    group_devs = lax.axis_size("kgrp")
    freq_total = per_freq * freq_devs
    pair_block = orbitals * orbitals // (freq_devs * group_devs)
    column = freq_devs // 2
    direct = (
        width == 128
        and per_freq == 2
        and freq_devs % 2 == 0
        and group_devs % 2 == 0
        and pair_block == width
        and column == 4
        and k_local == 8
        and weights.shape[0] % width == 0
    )
    if direct:
        table = weights.reshape(-1, width)
        hamiltonians, sigma_guess = gather(hamiltonian, self_energy, guess_factor, column)
        part = newton(hamiltonians, sigma_guess, table, counts)
        return scatter(part, table, freq_devs, group_devs)
    sigma = lax.all_gather(self_energy, "freq", axis=0, tiled=True)
    guess = lax.all_gather(guess_factor, "freq", axis=0, tiled=True)
    current, factors = early_steps(counts, weights, hamiltonian, sigma, guess)
    terms = local_sum(factors, hamiltonian, sigma, current)
    terms = terms.reshape(freq_total, orbitals, 2, orbitals).transpose(1, 3, 2, 0)
    terms = terms.reshape(orbitals * orbitals, 2 * freq_total)
    result = lax.psum_scatter(terms, ("freq", "kgrp"), scatter_dimension=0, tiled=True)
    return result.reshape(pair_block, 2 * freq_total)


def solution(mesh):
    return jax.shard_map(
        per_device,
        mesh=mesh,
        in_specs=(
            P(("freq", "kgrp"), None, None),
            P("freq", None, None),
            P("freq", None, None),
            P(),
            P(),
        ),
        out_specs=P(("freq", "kgrp"), None),
        check_vma=False,
    )
```

```python
import functools
import math

import jax
import jax.numpy as jnp
from jax import lax
from jax.experimental import pallas as pl
from jax.experimental.pallas import tpu as pltpu
from jax.sharding import PartitionSpec as P

chem_potential = 0.2
MESH = pl.DeviceIdType.MESH
GRANT = 32 * 1024 * 1024
VMEM = pl.BlockSpec(memory_space=pltpu.VMEM)
SMEM = pl.BlockSpec(memory_space=pltpu.SMEM)
HBM = pl.BlockSpec(memory_space=pltpu.HBM)
SPAN = 4


def split(value):
    high = value.astype(jnp.bfloat16).astype(jnp.float32)
    return high, value - high


def left_operand(value, half, left):
    high, low = split(value)
    turned_high, turned_low = split(pltpu.roll(value, half, 1))
    top = jnp.where(left, high, turned_low)
    bottom = jnp.where(left, turned_high, low)
    return jnp.concatenate([top, bottom], 0).astype(jnp.bfloat16)


def right_operand(value):
    high, low = split(value)
    row = jnp.concatenate([high, low], 1).astype(jnp.bfloat16)
    return jnp.concatenate([row, row], 0)


def fold(product, orbitals, sign):
    width = 2 * orbitals
    both = product[:, :width] + product[:, width:]
    return both[:orbitals] + sign * pltpu.roll(both[orbitals:], orbitals, 1)


def masks(shape):
    orbitals = shape[0]
    row = lax.broadcasted_iota(jnp.int32, shape, 0)
    lane = lax.broadcasted_iota(jnp.int32, shape, 1)
    left = lane < orbitals
    sign = jnp.where(left, -1.0, 1.0)
    eye_real = (lane == row).astype(jnp.float32)
    eye_imag = (lane == row + orbitals).astype(jnp.float32)
    return left, sign, eye_real, eye_imag


def shifted(freq, freq_total, eye_real, eye_imag, sigma):
    matsubara = (2 * freq + 1).astype(jnp.float32) * (math.pi / (2 * freq_total))
    return (chem_potential * eye_real + matsubara * eye_imag) - sigma


def steps_kernel(counts, weights, h_ref, sigma_ref, guess_ref, x_ref, factor_ref, m_left, h_diag):
    k_local, orbitals, width = h_ref.shape
    freq_total = sigma_ref.shape[0]
    shape = (orbitals, width)
    left, sign, eye_real, eye_imag = masks(shape)
    device = lax.axis_index("freq") * lax.axis_size("kgrp") + lax.axis_index("kgrp")

    def add_weight(index, total):
        return total + weights[index]

    weight_total = lax.fori_loop(
        0, weights.shape[0], add_weight, jnp.int32(0), unroll=8
    ).astype(jnp.float32)
    for k in range(k_local):
        weight = weights[device * k_local + k].astype(jnp.float32)
        factor_ref[k : k + 1, :] = jnp.full((1, width), weight) / weight_total

    def diagonal(value):
        real = jnp.sum(value * eye_real, axis=1, keepdims=True)
        imag = jnp.sum(value * eye_imag, axis=1, keepdims=True)
        return jnp.broadcast_to(real, shape), jnp.broadcast_to(imag, shape)

    for k in range(k_local):
        h_diag[0, k], h_diag[1, k] = diagonal(h_ref[k])

    def one_frequency(freq, carry):
        base = shifted(freq, freq_total, eye_real, eye_imag, sigma_ref[freq])
        base_real, base_imag = diagonal(base)
        guess = guess_ref[freq]
        turned = sign * pltpu.roll(guess, orbitals, 1)
        for k in range(k_local):
            real = base_real - h_diag[0, k]
            imag = base_imag - h_diag[1, k]
            inverse = 1.0 / (real * real + imag * imag)
            x_ref[freq, k] = (real * inverse) * guess - (imag * inverse) * turned

        @pl.when(counts[freq] > 1)
        def _():
            for k in range(k_local):
                m_left[k] = left_operand(base - h_ref[k], orbitals, left)

            def newton_step(sweep, inner):
                products = [
                    jnp.dot(
                        m_left[k],
                        right_operand(x_ref[freq, k]),
                        preferred_element_type=jnp.float32,
                    )
                    for k in range(k_local)
                ]
                products = [
                    jnp.dot(
                        left_operand(x_ref[freq, k], orbitals, left),
                        right_operand(eye_real - fold(products[k], orbitals, sign)),
                        preferred_element_type=jnp.float32,
                    )
                    for k in range(k_local)
                ]
                for k in range(k_local):
                    x_ref[freq, k] = x_ref[freq, k] + fold(products[k], orbitals, sign)
                return inner

            lax.fori_loop(0, counts[freq] - 1, newton_step, 0)

        return carry

    lax.fori_loop(0, freq_total, one_frequency, 0)


def early_steps(counts, weights, hamiltonian, sigma, guess):
    k_local, orbitals, width = hamiltonian.shape
    freq_total = sigma.shape[0]
    return pl.pallas_call(
        steps_kernel,
        out_shape=(
            jax.ShapeDtypeStruct((freq_total, k_local, orbitals, width), jnp.float32),
            jax.ShapeDtypeStruct((k_local, width), jnp.float32),
        ),
        in_specs=[SMEM, SMEM, VMEM, VMEM, VMEM],
        out_specs=(VMEM, VMEM),
        scratch_shapes=[
            pltpu.VMEM((k_local, width, width), jnp.bfloat16),
            pltpu.VMEM((2, k_local, orbitals, width), jnp.float32),
        ],
        compiler_params=pltpu.CompilerParams(vmem_limit_bytes=GRANT),
        name="early_steps",
    )(counts, weights, hamiltonian, sigma, guess)


def last_step(freq, freq_total, factor_ref, h_ref, sigma_ref, x_ref, last_left, last_right):
    k_local, orbitals, width = h_ref.shape
    left, sign, eye_real, eye_imag = masks((orbitals, width))
    base = shifted(freq, freq_total, eye_real, eye_imag, sigma_ref[freq])
    products = [
        jnp.dot(
            left_operand(base - h_ref[k], orbitals, left),
            right_operand(x_ref[freq, k]),
            preferred_element_type=jnp.float32,
        )
        for k in range(k_local)
    ]
    total = jnp.zeros((orbitals, width), jnp.float32)
    for k in range(k_local):
        weighted = x_ref[freq, k] * factor_ref[k : k + 1, :]
        last_left[:, k * width : (k + 1) * width] = left_operand(weighted, orbitals, left)
        total = total + weighted
    for k in range(k_local):
        missing = eye_real - fold(products[k], orbitals, sign)
        last_right[k * width : (k + 1) * width, :] = right_operand(missing)
    product = jnp.dot(last_left[...], last_right[...], preferred_element_type=jnp.float32)
    return total + fold(product, orbitals, sign)


def last_scratch(k_local, width):
    return [
        pltpu.VMEM((width, k_local * width), jnp.bfloat16),
        pltpu.VMEM((k_local * width, 2 * width), jnp.bfloat16),
    ]


def sum_kernel(factor_ref, h_ref, sigma_ref, x_ref, out_ref, last_left, last_right):
    freq_total = sigma_ref.shape[0]

    def one_frequency(freq, carry):
        out_ref[freq] = last_step(
            freq, freq_total, factor_ref, h_ref, sigma_ref, x_ref, last_left, last_right
        )
        return carry

    lax.fori_loop(0, freq_total, one_frequency, 0)


def local_sum(factors, hamiltonian, sigma, current):
    k_local, orbitals, width = hamiltonian.shape
    return pl.pallas_call(
        sum_kernel,
        out_shape=jax.ShapeDtypeStruct(sigma.shape, jnp.float32),
        in_specs=[VMEM] * 4,
        out_specs=VMEM,
        scratch_shapes=last_scratch(k_local, width),
        name="local_sum",
    )(factors, hamiltonian, sigma, current)


def halves(value):
    high = value.astype(jnp.bfloat16)
    return high, (value - high.astype(jnp.float32)).astype(jnp.bfloat16)


def turned_part(part, flip):
    half = part.shape[1] // 2
    return flip * pltpu.roll(part, half, 1)


def operand(high, low, flip):
    top = jnp.concatenate([high, low], 1)
    bottom = jnp.concatenate([turned_part(high, flip), turned_part(low, flip)], 1)
    return jnp.concatenate([top, bottom], 0)


def twice(part):
    return jnp.concatenate([part, part], 0)


def joined(product):
    width = product.shape[1] // 2
    return product[:, :width] + product[:, width:]


def dot(left_side, right_side):
    return jnp.dot(left_side, right_side, preferred_element_type=jnp.float32)


def gather_kernel(
    h_hbm,
    sigma_hbm,
    guess_hbm,
    weights_hbm,
    f_out,
    rows_out,
    sg_out,
    own_h,
    packed,
    weights,
    right_ref,
    g_side,
    g_shift,
    shift_rows,
    h_rows,
    scales,
    local,
    mate_sem,
    pair_sem,
    pass_sem,
    col_sem,
):
    column, slots, k_local, orbitals, width = f_out.shape
    pairs = k_local // 2
    shape = (orbitals, width)
    freq_devs = 2 * column
    freq_total = 2 * freq_devs
    me = lax.axis_index("freq")
    group = lax.axis_index("kgrp")
    group_devs = lax.axis_size("kgrp")
    parity = lax.rem(group, 2)
    branch = lax.rem(me, 2)
    place = me // 2
    pair = me + 1 - 2 * branch
    mate = group + 1 - 2 * parity
    others = [place + 1 - 2 * lax.rem(place, 2), lax.rem(place + 2, column), column - 1 - place]
    barrier = pltpu.get_barrier_semaphore()
    for other in others:
        pl.semaphore_signal(barrier, inc=1, device_id=(2 * other + branch, group), device_id_type=MESH)
    pl.semaphore_signal(barrier, inc=1, device_id=(pair, group), device_id_type=MESH)
    pl.semaphore_signal(barrier, inc=1, device_id=(me, mate), device_id_type=MESH)
    loads = [
        pltpu.make_async_copy(h_hbm, own_h, local.at[0]),
        pltpu.make_async_copy(sigma_hbm.at[parity], sg_out.at[place, 0], local.at[1]),
        pltpu.make_async_copy(guess_hbm.at[parity], sg_out.at[place, 1], local.at[2]),
        pltpu.make_async_copy(weights_hbm, weights, local.at[3]),
    ]
    for load in loads:
        load.start()

    def remote(src, dst, sems, slot, freq_to, group_to):
        return pltpu.make_async_remote_copy(
            src_ref=src,
            dst_ref=dst,
            send_sem=sems.at[0, slot],
            recv_sem=sems.at[1, slot],
            device_id=(freq_to, group_to),
            device_id_type=MESH,
        )

    own = sg_out.at[place]
    columns = [
        remote(own, own, col_sem, index, 2 * others[index] + branch, group) for index in range(column - 1)
    ]
    across = [remote(packed.at[0, c], packed.at[2, c], pair_sem, c, pair, group) for c in range(pairs)]
    passes = [remote(packed.at[2, c], packed.at[3, c], pass_sem, c, me, mate) for c in range(pairs)]
    beside = remote(packed.at[0], packed.at[1], mate_sem, 0, me, mate)

    row = lax.broadcasted_iota(jnp.int32, shape, 0)
    lane = lax.broadcasted_iota(jnp.int32, shape, 1)
    left = lane < orbitals
    within = jnp.where(left, lane, lane - orbitals)
    upper = within >= row
    above = within > row
    flip = jnp.where(lax.broadcasted_iota(jnp.int32, shape, 1) < orbitals, -1.0, 1.0).astype(jnp.bfloat16)
    eye_real = (lane == row).astype(jnp.float32)
    eye_imag = (lane == row + orbitals).astype(jnp.float32)
    eye_both = (within == row).astype(jnp.float32)

    def turn(value):
        return pltpu.roll(value, orbitals, 1)

    loads[0].wait()
    for c in range(pairs):
        one, two = own_h[2 * c], own_h[2 * c + 1]
        real = jnp.where(left, one, turn(two))
        imag = jnp.where(left, turn(one), two)
        packed[0, c] = jnp.where(upper, real, imag)
    loads[1].wait()
    loads[2].wait()
    pl.semaphore_wait(barrier, column + 1)
    for copy in across + columns + [beside]:
        copy.start()
    loads[3].wait()

    def prepare(index):
        frequency = 2 * (2 * index + branch) + parity
        base = shifted(frequency, freq_total, eye_real, eye_imag, sg_out[index, 0])
        guess = sg_out[index, 1]
        guess_side = jnp.concatenate(halves(guess), 1)
        g_side[index] = guess_side
        swapped = turn(base)
        real = jnp.sum(eye_real * base + eye_imag * swapped, axis=0, keepdims=True)
        imag = jnp.sum(eye_real * swapped + eye_imag * base, axis=0, keepdims=True)
        shift_rows[index, 0] = jnp.broadcast_to(real, (k_local, width))
        shift_rows[index, 1] = jnp.broadcast_to(imag, (k_local, width))
        high, low = halves(base)
        g_shift[index] = joined(dot(guess_side, twice(operand(high, low, flip))))

    def unpack(slot):
        diagonals = []
        for c in range(pairs):
            value = packed[slot, c]
            flipped = jnp.transpose(value)
            other = jnp.concatenate([flipped[:orbitals], flipped[orbitals:]], 1)
            real = jnp.where(upper, value, other)
            imag = jnp.where(above, -other, jnp.where(upper, 0.0, value))
            real_turned, imag_turned = turn(real), turn(imag)
            diagonal = jnp.sum(eye_both * value, axis=0, keepdims=True)
            swapped = pltpu.roll(jnp.broadcast_to(diagonal, (8, width)), orbitals, 1)[:1]
            left_row = left[:1]
            diagonals.append(jnp.where(left_row, diagonal, swapped))
            diagonals.append(jnp.where(left_row, swapped, diagonal))
            tops = jnp.where(left, real, imag_turned), jnp.where(left, real_turned, imag)
            bottoms = jnp.where(left, -imag, real_turned), jnp.where(left, -imag_turned, real)
            for offset in range(2):
                right_ref[slot, 2 * c + offset, :orbitals] = jnp.concatenate(halves(tops[offset]), 1)
                right_ref[slot, 2 * c + offset, orbitals:] = jnp.concatenate(halves(bottoms[offset]), 1)
        h_rows[slot] = jnp.concatenate(diagonals, 0)

    tile = (k_local, width)
    k_row = lax.broadcasted_iota(jnp.int32, tile, 0)
    tile_left = lax.broadcasted_iota(jnp.int32, tile, 1) < orbitals

    def slot_weights(slot):
        owner_freq = me + (slot // 2) * (1 - 2 * branch)
        owner_group = group + (slot % 2) * (1 - 2 * parity)
        k_first = (owner_freq * group_devs + owner_group) * k_local
        first_row, first_column = lax.div(k_first, width), lax.rem(k_first, width)
        weight = jnp.zeros(tile, jnp.float32)
        for j in range(k_local):
            value = weights[first_row, first_column + j].astype(jnp.float32)
            weight = jnp.where(k_row == j, value, weight)
        return weight

    def apply(at_slots, indices):
        for slot in at_slots:
            weight = slot_weights(slot)
            for index in indices:
                real = shift_rows[index, 0] - h_rows[slot]
                imag = shift_rows[index, 1]
                inverse = 1.0 / (real * real + imag * imag)
                d_real = real * inverse
                d_imag = -imag * inverse
                scales[index, slot, 0] = d_real
                scales[index, slot, 1] = jnp.where(tile_left, -d_imag, d_imag)
                rows_out[index, slot] = weight * jnp.where(tile_left, d_real, d_imag)
        side = jnp.concatenate([g_side[index] for index in indices], 0)
        for slot in at_slots:
            for j in range(k_local):
                product = joined(dot(side, twice(right_ref[slot, j])))
                for at, index in enumerate(indices):
                    q = g_shift[index] - product[at * orbitals : (at + 1) * orbitals]
                    d_real = scales[index, slot, 0, j : j + 1, :]
                    d_imag = scales[index, slot, 1, j : j + 1, :]
                    f_out[index, slot, j] = eye_real - q * d_real - turn(q) * d_imag

    prepare(place)
    unpack(0)
    apply([0], [place])
    beside.wait_recv()
    unpack(1)
    apply([1], [place])
    for index in range(column - 2):
        columns[index].wait_recv()
        prepare(others[index])
        apply([0, 1], [others[index]])
        for c in range(2 * index, 2 * index + 2):
            across[c].wait_recv()
            passes[c].start()
    early = [place] + others[:-1]
    unpack(2)
    apply([2], early)
    for copy in passes:
        copy.wait_recv()
    unpack(3)
    apply([3], early)
    columns[-1].wait_recv()
    prepare(others[-1])
    apply(range(slots), [others[-1]])
    for copy in columns + across + passes + [beside]:
        copy.wait_send()


def gather(hamiltonian, self_energy, guess_factor, weights, column):
    k_local, orbitals, width = hamiltonian.shape
    pairs = k_local // 2
    return pl.pallas_call(
        gather_kernel,
        out_shape=(
            jax.ShapeDtypeStruct((column, 4, k_local, orbitals, width), jnp.float32),
            jax.ShapeDtypeStruct((column, 4, k_local, width), jnp.float32),
            jax.ShapeDtypeStruct((column, 2, orbitals, width), jnp.float32),
        ),
        in_specs=[HBM] * 4,
        out_specs=(VMEM,) * 3,
        scratch_shapes=[
            pltpu.VMEM((k_local, orbitals, width), jnp.float32),
            pltpu.VMEM((4, pairs, orbitals, width), jnp.float32),
            pltpu.SMEM(weights.shape, jnp.int32),
            pltpu.VMEM((4, k_local, width, 2 * width), jnp.bfloat16),
            pltpu.VMEM((column, orbitals, 2 * width), jnp.bfloat16),
            pltpu.VMEM((column, orbitals, width), jnp.float32),
            pltpu.VMEM((column, 2, k_local, width), jnp.float32),
            pltpu.VMEM((4, k_local, width), jnp.float32),
            pltpu.VMEM((column, 4, 2, k_local, width), jnp.float32),
            pltpu.SemaphoreType.DMA((4,)),
            pltpu.SemaphoreType.DMA((2, 1)),
            pltpu.SemaphoreType.DMA((2, pairs)),
            pltpu.SemaphoreType.DMA((2, pairs)),
            pltpu.SemaphoreType.DMA((2, column)),
        ],
        compiler_params=pltpu.CompilerParams(collective_id=0, has_side_effects=True, vmem_limit_bytes=GRANT),
        name="gather",
    )(hamiltonian, self_energy, guess_factor, weights)


def newton_kernel(f_ref, rows, sg_ref, counts_hbm, out_ref, counts, load_sem, left_ref, right_ref, work, total_ref):
    column, slots, k_local, orbitals, width = f_ref.shape
    span = work.shape[1]
    per_step = span // k_local
    shape = (orbitals, width)
    me = lax.axis_index("freq")
    parity = lax.rem(lax.axis_index("kgrp"), 2)
    branch = lax.rem(me, 2)
    load = pltpu.make_async_copy(counts_hbm, counts, load_sem.at[0])
    load.start()
    lane = lax.broadcasted_iota(jnp.int32, shape, 1)
    flip = jnp.where(lane < orbitals, -1.0, 1.0).astype(jnp.bfloat16)
    eye_real = (lane == lax.broadcasted_iota(jnp.int32, shape, 0)).astype(jnp.float32)
    sign = jnp.where(lane < orbitals, -1.0, 1.0)
    eye_half = (lax.rem(lane, orbitals) == lax.broadcasted_iota(jnp.int32, shape, 0)).astype(jnp.bfloat16)
    load.wait()

    def turn(value):
        return pltpu.roll(value, orbitals, 1)

    def block(value):
        high, low = halves(value)
        return operand(high, low, flip)

    def side(value):
        return jnp.concatenate(halves(value), 1)

    def one_frequency(index, carry):
        count = counts[2 * (2 * index + branch) + parity]

        def at(step, k):
            return index, step * per_step + k // k_local, k % k_local

        def accumulate():
            product = dot(left_ref[...], right_ref[...])
            total_ref[...] += joined(product[:orbitals]) + product[orbitals:, :width]

        def store_left(k, high, low):
            left_ref[:orbitals, k * width : (k + 1) * width] = high
            left_ref[orbitals:, k * width : (k + 1) * width] = low

        def store_right(k, value):
            right_ref[k * width : (k + 1) * width, :] = block(value)

        total_ref[...] = jnp.zeros(shape, jnp.float32)

        @pl.when(count == 1)
        def _():
            def sweep(step, inner):
                for k in range(span):
                    _, slot, j = at(step, k)
                    if j == 0:
                        row_high, row_low = halves(rows[index, slot])
                    store_left(k, eye_half * row_high[j : j + 1, :], eye_half * row_low[j : j + 1, :])
                    store_right(k, eye_real + f_ref[at(step, k)])
                accumulate()
                return inner

            lax.fori_loop(0, slots // per_step, sweep, 0)

        def squares(step):
            for k in range(span):
                value = f_ref[at(step, k)]
                high, low = halves(value)
                both = jnp.concatenate([high, low], 1)
                work[0, k] = joined(dot(both, twice(operand(high, low, flip))))

        def finish(step, outer, inner):
            for k in range(span):
                _, slot, j = at(step, k)
                if j == 0:
                    flat = jnp.transpose(rows[index, slot])
                d_real = jnp.broadcast_to(flat[:orbitals, j : j + 1], shape)
                d_imag = jnp.broadcast_to(flat[orbitals:, j : j + 1], shape)
                value = outer(k)
                store_left(k, *halves(d_real * value + d_imag * (sign * turn(value))))
                store_right(k, eye_real + inner(k))
            accumulate()

        @pl.when(count == 2)
        def _():
            def sweep(step, inner):
                squares(step)
                finish(step, lambda k: eye_real + f_ref[at(step, k)], lambda k: work[0, k])
                return inner

            lax.fori_loop(0, slots // per_step, sweep, 0)

        @pl.when(count > 2)
        def _():
            def sweep(step, inner):
                squares(step)
                for k in range(span):
                    value = f_ref[at(step, k)]
                    square = work[0, k]
                    high, low = halves(square)
                    both = jnp.concatenate([side(value), jnp.concatenate([high, low], 1)], 0)
                    product = joined(dot(both, twice(operand(high, low, flip))))
                    work[1, k] = eye_real + value + square + product[:orbitals]
                    work[2, k] = product[orbitals:]
                finish(step, lambda k: work[1, k], lambda k: work[2, k])
                return inner

            lax.fori_loop(0, slots // per_step, sweep, 0)

        green = joined(dot(side(total_ref[...]), twice(block(sg_ref[index, 1]))))
        out_ref[pl.ds(index, orbitals, stride=column), :] = green
        return carry

    lax.fori_loop(0, column, one_frequency, 0)


def newton(f_values, rows, sigma_guess, counts):
    column, slots, k_local, orbitals, width = f_values.shape
    span = SPAN * k_local
    return pl.pallas_call(
        newton_kernel,
        out_shape=jax.ShapeDtypeStruct((column * orbitals, width), jnp.float32),
        in_specs=[VMEM, VMEM, VMEM, HBM],
        out_specs=VMEM,
        scratch_shapes=[
            pltpu.SMEM(counts.shape, jnp.int32),
            pltpu.SemaphoreType.DMA((1,)),
            pltpu.VMEM((2 * orbitals, span * width), jnp.bfloat16),
            pltpu.VMEM((span * width, 2 * width), jnp.bfloat16),
            pltpu.VMEM((3, span, orbitals, width), jnp.float32),
            pltpu.VMEM((orbitals, width), jnp.float32),
        ],
        compiler_params=pltpu.CompilerParams(vmem_limit_bytes=GRANT),
        name="newton",
    )(f_values, rows, sigma_guess, counts)


def scatter_kernel(part, weights_hbm, out_ref, weights, landed, load_sem, send, recv):
    freq_devs = lax.axis_size("freq")
    group_devs = lax.axis_size("kgrp")
    column = freq_devs // 2
    tile, width = landed.shape[2:]
    orbitals = width // 2
    me = lax.axis_index("freq")
    group = lax.axis_index("kgrp")
    others = [(a, b) for a in range(freq_devs) for b in range(group_devs) if a + b > 0]
    barrier = pltpu.get_barrier_semaphore()

    def place(step):
        return lax.rem(me + step[0], freq_devs), lax.rem(group + step[1], group_devs)

    for step in others:
        pl.semaphore_signal(barrier, inc=1, device_id=place(step), device_id_type=MESH)
    load = pltpu.make_async_copy(weights_hbm, weights, load_sem.at[0])
    load.start()

    def spread(index):
        freq_to, group_to = place(others[index])
        return pltpu.make_async_remote_copy(
            src_ref=part.at[pl.ds((freq_to * group_devs + group_to) * tile, tile)],
            dst_ref=landed.at[me, group],
            send_sem=send.at[index],
            recv_sem=recv.at[index],
            device_id=(freq_to, group_to),
            device_id_type=MESH,
        )

    pl.semaphore_wait(barrier, len(others))
    for index in range(len(others)):
        spread(index).start()
    landed[me, group] = part[pl.ds((me * group_devs + group) * tile, tile), :]
    load.wait()
    total = jnp.sum(weights[...].astype(jnp.float32), axis=0, keepdims=True)
    scale = 1.0 / jnp.broadcast_to(jnp.sum(total, axis=1, keepdims=True), (tile, width))
    for index in range(len(others)):
        spread(index).wait_recv()
    left = lax.broadcasted_iota(jnp.int32, (tile, width), 1) < orbitals
    freq_total = 4 * column
    for branch in range(2):
        for parity in range(2):
            total = None
            for place_at in range(column):
                for high in range(group_devs // 2):
                    term = landed[2 * place_at + branch, 2 * high + parity]
                    total = term if total is None else total + term
            total = total * scale
            swapped = pltpu.roll(total, tile // 2, 0)
            turned = pltpu.roll(total, orbitals, 1)
            turned_swapped = pltpu.roll(turned, tile // 2, 0)
            real = jnp.where(left, total, turned_swapped)
            imag = jnp.where(left, turned, swapped)
            first = 2 * branch + parity
            out_ref[pl.ds(first, column, stride=4), :] = real[:column]
            out_ref[pl.ds(freq_total + first, column, stride=4), :] = imag[:column]
    for index in range(len(others)):
        spread(index).wait_send()


def scatter(part, weights, freq_devs, group_devs):
    width = part.shape[1]
    tile = part.shape[0] // (freq_devs * group_devs)
    column = freq_devs // 2
    peers = freq_devs * group_devs - 1
    return pl.pallas_call(
        scatter_kernel,
        out_shape=jax.ShapeDtypeStruct((8 * column, width), jnp.float32),
        in_specs=[VMEM, HBM],
        out_specs=VMEM,
        scratch_shapes=[
            pltpu.VMEM(weights.shape, jnp.int32),
            pltpu.VMEM((freq_devs, group_devs, tile, width), jnp.float32),
            pltpu.SemaphoreType.DMA((1,)),
            pltpu.SemaphoreType.DMA((peers,)),
            pltpu.SemaphoreType.DMA((peers,)),
        ],
        compiler_params=pltpu.CompilerParams(collective_id=1, has_side_effects=True, vmem_limit_bytes=GRANT),
        name="scatter",
    )(part, weights)


def per_device(hamiltonian, self_energy, guess_factor, weights, counts):
    k_local, orbitals, width = hamiltonian.shape
    per_freq = self_energy.shape[0]
    freq_devs = lax.axis_size("freq")
    group_devs = lax.axis_size("kgrp")
    freq_total = per_freq * freq_devs
    pair_block = orbitals * orbitals // (freq_devs * group_devs)
    column = freq_devs // 2
    direct = (
        width == 128
        and per_freq == 2
        and freq_devs % 2 == 0
        and group_devs % 2 == 0
        and pair_block == width
        and column == 4
        and k_local == 8
        and weights.shape[0] % width == 0
    )
    if direct:
        table = weights.reshape(-1, width)
        inputs = [
            pltpu.with_memory_space_constraint(value, pltpu.HBM)
            for value in (hamiltonian, self_energy, guess_factor, table)
        ]
        table = inputs[3]
        counts = pltpu.with_memory_space_constraint(counts, pltpu.HBM)
        values, rows, sigma_guess = gather(*inputs, column)
        part = newton(values, rows, sigma_guess, counts)
        return scatter(part, table, freq_devs, group_devs).T
    sigma = lax.all_gather(self_energy, "freq", axis=0, tiled=True)
    guess = lax.all_gather(guess_factor, "freq", axis=0, tiled=True)
    current, factors = early_steps(counts, weights, hamiltonian, sigma, guess)
    terms = local_sum(factors, hamiltonian, sigma, current)
    terms = terms.reshape(freq_total, orbitals, 2, orbitals).transpose(1, 3, 2, 0)
    terms = terms.reshape(orbitals * orbitals, 2 * freq_total)
    result = lax.psum_scatter(terms, ("freq", "kgrp"), scatter_dimension=0, tiled=True)
    return result.reshape(pair_block, 2 * freq_total)


def solution(mesh):
    return jax.shard_map(
        per_device,
        mesh=mesh,
        in_specs=(
            P(("freq", "kgrp"), None, None),
            P("freq", None, None),
            P("freq", None, None),
            P(),
            P(),
        ),
        out_specs=P(("freq", "kgrp"), None),
        check_vma=False,
    )
```

```python
import functools
import math

import jax
import jax.numpy as jnp
from jax import lax
from jax.experimental import pallas as pl
from jax.experimental.pallas import tpu as pltpu
from jax.sharding import PartitionSpec as P

chem_potential = 0.2
MESH = pl.DeviceIdType.MESH
GRANT = 32 * 1024 * 1024
VMEM = pl.BlockSpec(memory_space=pltpu.VMEM)
SMEM = pl.BlockSpec(memory_space=pltpu.SMEM)
HBM = pl.BlockSpec(memory_space=pltpu.HBM)
LAG = 2


def split(value):
    high = value.astype(jnp.bfloat16).astype(jnp.float32)
    return high, value - high


def left_operand(value, half, left):
    high, low = split(value)
    turned_high, turned_low = split(pltpu.roll(value, half, 1))
    top = jnp.where(left, high, turned_low)
    bottom = jnp.where(left, turned_high, low)
    return jnp.concatenate([top, bottom], 0).astype(jnp.bfloat16)


def right_operand(value):
    high, low = split(value)
    row = jnp.concatenate([high, low], 1).astype(jnp.bfloat16)
    return jnp.concatenate([row, row], 0)


def fold(product, orbitals, sign):
    width = 2 * orbitals
    both = product[:, :width] + product[:, width:]
    return both[:orbitals] + sign * pltpu.roll(both[orbitals:], orbitals, 1)


def masks(shape):
    orbitals = shape[0]
    row = lax.broadcasted_iota(jnp.int32, shape, 0)
    lane = lax.broadcasted_iota(jnp.int32, shape, 1)
    left = lane < orbitals
    sign = jnp.where(left, -1.0, 1.0)
    eye_real = (lane == row).astype(jnp.float32)
    eye_imag = (lane == row + orbitals).astype(jnp.float32)
    return left, sign, eye_real, eye_imag


def shifted(freq, freq_total, eye_real, eye_imag, sigma):
    matsubara = (2 * freq + 1).astype(jnp.float32) * (math.pi / (2 * freq_total))
    return (chem_potential * eye_real + matsubara * eye_imag) - sigma


def steps_kernel(counts, weights, h_ref, sigma_ref, guess_ref, x_ref, factor_ref, m_left, h_diag):
    k_local, orbitals, width = h_ref.shape
    freq_total = sigma_ref.shape[0]
    shape = (orbitals, width)
    left, sign, eye_real, eye_imag = masks(shape)
    device = lax.axis_index("freq") * lax.axis_size("kgrp") + lax.axis_index("kgrp")

    def add_weight(index, total):
        return total + weights[index]

    weight_total = lax.fori_loop(
        0, weights.shape[0], add_weight, jnp.int32(0), unroll=8
    ).astype(jnp.float32)
    for k in range(k_local):
        weight = weights[device * k_local + k].astype(jnp.float32)
        factor_ref[k : k + 1, :] = jnp.full((1, width), weight) / weight_total

    def diagonal(value):
        real = jnp.sum(value * eye_real, axis=1, keepdims=True)
        imag = jnp.sum(value * eye_imag, axis=1, keepdims=True)
        return jnp.broadcast_to(real, shape), jnp.broadcast_to(imag, shape)

    for k in range(k_local):
        h_diag[0, k], h_diag[1, k] = diagonal(h_ref[k])

    def one_frequency(freq, carry):
        base = shifted(freq, freq_total, eye_real, eye_imag, sigma_ref[freq])
        base_real, base_imag = diagonal(base)
        guess = guess_ref[freq]
        turned = sign * pltpu.roll(guess, orbitals, 1)
        for k in range(k_local):
            real = base_real - h_diag[0, k]
            imag = base_imag - h_diag[1, k]
            inverse = 1.0 / (real * real + imag * imag)
            x_ref[freq, k] = (real * inverse) * guess - (imag * inverse) * turned

        @pl.when(counts[freq] > 1)
        def _():
            for k in range(k_local):
                m_left[k] = left_operand(base - h_ref[k], orbitals, left)

            def newton_step(sweep, inner):
                products = [
                    jnp.dot(
                        m_left[k],
                        right_operand(x_ref[freq, k]),
                        preferred_element_type=jnp.float32,
                    )
                    for k in range(k_local)
                ]
                products = [
                    jnp.dot(
                        left_operand(x_ref[freq, k], orbitals, left),
                        right_operand(eye_real - fold(products[k], orbitals, sign)),
                        preferred_element_type=jnp.float32,
                    )
                    for k in range(k_local)
                ]
                for k in range(k_local):
                    x_ref[freq, k] = x_ref[freq, k] + fold(products[k], orbitals, sign)
                return inner

            lax.fori_loop(0, counts[freq] - 1, newton_step, 0)

        return carry

    lax.fori_loop(0, freq_total, one_frequency, 0)


def early_steps(counts, weights, hamiltonian, sigma, guess):
    k_local, orbitals, width = hamiltonian.shape
    freq_total = sigma.shape[0]
    return pl.pallas_call(
        steps_kernel,
        out_shape=(
            jax.ShapeDtypeStruct((freq_total, k_local, orbitals, width), jnp.float32),
            jax.ShapeDtypeStruct((k_local, width), jnp.float32),
        ),
        in_specs=[SMEM, SMEM, VMEM, VMEM, VMEM],
        out_specs=(VMEM, VMEM),
        scratch_shapes=[
            pltpu.VMEM((k_local, width, width), jnp.bfloat16),
            pltpu.VMEM((2, k_local, orbitals, width), jnp.float32),
        ],
        compiler_params=pltpu.CompilerParams(vmem_limit_bytes=GRANT),
        name="early_steps",
    )(counts, weights, hamiltonian, sigma, guess)


def last_step(freq, freq_total, factor_ref, h_ref, sigma_ref, x_ref, last_left, last_right):
    k_local, orbitals, width = h_ref.shape
    left, sign, eye_real, eye_imag = masks((orbitals, width))
    base = shifted(freq, freq_total, eye_real, eye_imag, sigma_ref[freq])
    products = [
        jnp.dot(
            left_operand(base - h_ref[k], orbitals, left),
            right_operand(x_ref[freq, k]),
            preferred_element_type=jnp.float32,
        )
        for k in range(k_local)
    ]
    total = jnp.zeros((orbitals, width), jnp.float32)
    for k in range(k_local):
        weighted = x_ref[freq, k] * factor_ref[k : k + 1, :]
        last_left[:, k * width : (k + 1) * width] = left_operand(weighted, orbitals, left)
        total = total + weighted
    for k in range(k_local):
        missing = eye_real - fold(products[k], orbitals, sign)
        last_right[k * width : (k + 1) * width, :] = right_operand(missing)
    product = jnp.dot(last_left[...], last_right[...], preferred_element_type=jnp.float32)
    return total + fold(product, orbitals, sign)


def last_scratch(k_local, width):
    return [
        pltpu.VMEM((width, k_local * width), jnp.bfloat16),
        pltpu.VMEM((k_local * width, 2 * width), jnp.bfloat16),
    ]


def sum_kernel(factor_ref, h_ref, sigma_ref, x_ref, out_ref, last_left, last_right):
    freq_total = sigma_ref.shape[0]

    def one_frequency(freq, carry):
        out_ref[freq] = last_step(
            freq, freq_total, factor_ref, h_ref, sigma_ref, x_ref, last_left, last_right
        )
        return carry

    lax.fori_loop(0, freq_total, one_frequency, 0)


def local_sum(factors, hamiltonian, sigma, current):
    k_local, orbitals, width = hamiltonian.shape
    return pl.pallas_call(
        sum_kernel,
        out_shape=jax.ShapeDtypeStruct(sigma.shape, jnp.float32),
        in_specs=[VMEM] * 4,
        out_specs=VMEM,
        scratch_shapes=last_scratch(k_local, width),
        name="local_sum",
    )(factors, hamiltonian, sigma, current)


def halves(value):
    high = value.astype(jnp.bfloat16)
    return high, (value - high.astype(jnp.float32)).astype(jnp.bfloat16)


def joined(product):
    width = product.shape[1] // 2
    return product[:, :width] + product[:, width:]


def dot(left_side, right_side):
    return jnp.dot(left_side, right_side, preferred_element_type=jnp.float32)


def grid_of(blocks):
    return jnp.concatenate([jnp.concatenate(line, 1) for line in blocks], 0)


def gather_kernel(
    h_hbm,
    sigma_hbm,
    guess_hbm,
    weights_hbm,
    counts_hbm,
    f_out,
    rows_out,
    sg_out,
    counts_out,
    own_h,
    packed,
    weights,
    right_ref,
    g_side,
    g_shift,
    shift_rows,
    h_rows,
    scales,
    local,
    mate_sem,
    pair_sem,
    pass_sem,
    col_sem,
):
    column, slots, pairs, _, orbitals, width = f_out.shape
    k_local = 2 * pairs
    shape = (orbitals, width)
    freq_devs = 2 * column
    freq_total = 2 * freq_devs
    me = lax.axis_index("freq")
    group = lax.axis_index("kgrp")
    group_devs = lax.axis_size("kgrp")
    parity = lax.rem(group, 2)
    branch = lax.rem(me, 2)
    place = me // 2
    pair = me + 1 - 2 * branch
    mate = group + 1 - 2 * parity
    others = [place + 1 - 2 * lax.rem(place, 2), lax.rem(place + 2, column), column - 1 - place]
    barrier = pltpu.get_barrier_semaphore()
    for other in others:
        pl.semaphore_signal(barrier, inc=1, device_id=(2 * other + branch, group), device_id_type=MESH)
    pl.semaphore_signal(barrier, inc=1, device_id=(pair, group), device_id_type=MESH)
    pl.semaphore_signal(barrier, inc=1, device_id=(me, mate), device_id_type=MESH)
    loads = [
        pltpu.make_async_copy(h_hbm, own_h, local.at[0]),
        pltpu.make_async_copy(sigma_hbm.at[parity], sg_out.at[place, 0], local.at[1]),
        pltpu.make_async_copy(guess_hbm.at[parity], sg_out.at[place, 1], local.at[2]),
        pltpu.make_async_copy(weights_hbm, weights, local.at[3]),
        pltpu.make_async_copy(counts_hbm, counts_out, local.at[4]),
    ]
    for load in loads:
        load.start()

    def remote(src, dst, sems, slot, freq_to, group_to):
        return pltpu.make_async_remote_copy(
            src_ref=src,
            dst_ref=dst,
            send_sem=sems.at[0, slot],
            recv_sem=sems.at[1, slot],
            device_id=(freq_to, group_to),
            device_id_type=MESH,
        )

    own = sg_out.at[place]
    columns = [
        remote(own, own, col_sem, index, 2 * others[index] + branch, group) for index in range(column - 1)
    ]
    across = [remote(packed.at[0, c], packed.at[2, c], pair_sem, c, pair, group) for c in range(pairs)]
    passes = [remote(packed.at[2, c], packed.at[3, c], pass_sem, c, me, mate) for c in range(pairs)]
    beside = remote(packed.at[0], packed.at[1], mate_sem, 0, me, mate)

    row = lax.broadcasted_iota(jnp.int32, shape, 0)
    lane = lax.broadcasted_iota(jnp.int32, shape, 1)
    left = lane < orbitals
    within = jnp.where(left, lane, lane - orbitals)
    upper = within >= row
    above = within > row
    eye_both = (within == row).astype(jnp.float32)

    def turn(value):
        return pltpu.roll(value, orbitals, 1)

    def planes(slot, c, real, imag):
        diagonal = jnp.sum(eye_both * real, axis=0, keepdims=True)
        h_rows[slot, c : c + 1, :] = diagonal
        h_rows[slot, pairs + c : pairs + c + 1, :] = diagonal
        for part, (r, i) in enumerate(zip(halves(real), halves(imag))):
            right_ref[slot, c, part] = grid_of([[r, i], [-i, r]])

    loads[0].wait()
    for c in range(pairs):
        one, two = own_h[2 * c], own_h[2 * c + 1]
        real = jnp.where(left, one, turn(two))
        imag = jnp.where(left, turn(one), two)
        packed[0, c] = jnp.where(upper, real, imag)
    loads[1].wait()
    loads[2].wait()
    pl.semaphore_wait(barrier, column + 1)
    for copy in across + columns + [beside]:
        copy.start()
    loads[3].wait()
    loads[4].wait()

    def times(guess_side, right_high, right_low):
        return dot(guess_side, jnp.concatenate([right_high, right_high, right_low], 0))

    def prepare(index):
        frequency = 2 * (2 * index + branch) + parity
        matsubara = (2 * frequency + 1).astype(jnp.float32) * (math.pi / (2 * freq_total))
        sigma = sg_out[index, 0]
        swapped = turn(sigma)
        real = chem_potential * eye_both - jnp.where(left, sigma, swapped)
        imag = matsubara * eye_both - jnp.where(left, swapped, sigma)
        high, low = halves(sg_out[index, 1])
        guess_side = jnp.concatenate([high, low, high], 1)
        g_side[index] = guess_side
        shift_rows[index, 0] = jnp.broadcast_to(jnp.sum(eye_both * real, axis=0, keepdims=True), tile)
        shift_rows[index, 1] = jnp.broadcast_to(jnp.sum(eye_both * imag, axis=0, keepdims=True), tile)
        (real_high, real_low), (imag_high, imag_low) = halves(real), halves(imag)
        product = times(
            guess_side,
            grid_of([[real_high, imag_high], [-imag_high, real_high]]),
            grid_of([[real_low, imag_low], [-imag_low, real_low]]),
        )
        g_shift[index] = product

    def unpack(slot):
        for c in range(pairs):
            value = packed[slot, c]
            flipped = jnp.transpose(value)
            other = jnp.concatenate([flipped[:orbitals], flipped[orbitals:]], 1)
            real = jnp.where(upper, value, other)
            imag = jnp.where(above, -other, jnp.where(upper, 0.0, value))
            planes(slot, c, real, imag)

    tile = (2 * pairs, width)
    tile_row = lax.broadcasted_iota(jnp.int32, tile, 0)
    tile_left = lax.broadcasted_iota(jnp.int32, tile, 1) < orbitals
    tile_real = tile_row < pairs
    tile_k = 2 * jnp.where(tile_real, tile_row, tile_row - pairs) + jnp.where(tile_left, 0, 1)

    def slot_weights(slot):
        owner_freq = me + (slot // 2) * (1 - 2 * branch)
        owner_group = group + (slot % 2) * (1 - 2 * parity)
        k_first = (owner_freq * group_devs + owner_group) * k_local
        first_row, first_column = lax.div(k_first, width), lax.rem(k_first, width)
        weight = jnp.zeros(tile, jnp.float32)
        for j in range(k_local):
            value = weights[first_row, first_column + j].astype(jnp.float32)
            weight = jnp.where(tile_k == j, value, weight)
        return weight

    def apply(at_slots, indices):
        for slot in at_slots:
            weight = slot_weights(slot)
            for index in indices:
                real = shift_rows[index, 0] - h_rows[slot]
                imag = shift_rows[index, 1]
                inverse = 1.0 / (real * real + imag * imag)
                scale = jnp.where(tile_real, real * inverse, -imag * inverse)
                scales[index, slot] = scale
                rows_out[index, slot] = weight * scale
        side = jnp.concatenate([g_side[index] for index in indices], 0)
        for slot in at_slots:
            for c in range(pairs):
                product = times(side, right_ref[slot, c, 0], right_ref[slot, c, 1])
                for at, index in enumerate(indices):
                    q = g_shift[index] - product[at * orbitals : (at + 1) * orbitals]
                    d_real = scales[index, slot, c : c + 1, :]
                    d_imag = scales[index, slot, pairs + c : pairs + c + 1, :]
                    real, imag = q[:, :width], q[:, width:]
                    f_out[index, slot, c, 0] = eye_both - real * d_real + imag * d_imag
                    f_out[index, slot, c, 1] = -real * d_imag - imag * d_real

    prepare(place)
    unpack(0)
    apply([0], [place])
    beside.wait_recv()
    unpack(1)
    apply([1], [place])
    for index in range(column - 2):
        columns[index].wait_recv()
        prepare(others[index])
        apply([0, 1], [others[index]])
        for c in range(2 * index, 2 * index + 2):
            across[c].wait_recv()
            passes[c].start()
    early = [place] + others[:-1]
    unpack(2)
    apply([2], early)
    for copy in passes:
        copy.wait_recv()
    unpack(3)
    apply([3], early)
    columns[-1].wait_recv()
    prepare(others[-1])
    apply(range(slots), [others[-1]])
    for copy in columns + across + passes + [beside]:
        copy.wait_send()


def gather(hamiltonian, self_energy, guess_factor, weights, counts, column):
    k_local, orbitals, width = hamiltonian.shape
    pairs = k_local // 2
    return pl.pallas_call(
        gather_kernel,
        out_shape=(
            jax.ShapeDtypeStruct((column, 4, pairs, 2, orbitals, width), jnp.float32),
            jax.ShapeDtypeStruct((column, 4, k_local, width), jnp.float32),
            jax.ShapeDtypeStruct((column, 2, orbitals, width), jnp.float32),
            jax.ShapeDtypeStruct(counts.shape, jnp.int32),
        ),
        in_specs=[HBM] * 5,
        out_specs=(VMEM,) * 4,
        scratch_shapes=[
            pltpu.VMEM((k_local, orbitals, width), jnp.float32),
            pltpu.VMEM((4, pairs, orbitals, width), jnp.float32),
            pltpu.SMEM(weights.shape, jnp.int32),
            pltpu.VMEM((4, pairs, 2, width, 2 * width), jnp.bfloat16),
            pltpu.VMEM((column, orbitals, 3 * width), jnp.bfloat16),
            pltpu.VMEM((column, orbitals, 2 * width), jnp.float32),
            pltpu.VMEM((column, 2, k_local, width), jnp.float32),
            pltpu.VMEM((4, k_local, width), jnp.float32),
            pltpu.VMEM((column, 4, k_local, width), jnp.float32),
            pltpu.SemaphoreType.DMA((5,)),
            pltpu.SemaphoreType.DMA((2, 1)),
            pltpu.SemaphoreType.DMA((2, pairs)),
            pltpu.SemaphoreType.DMA((2, pairs)),
            pltpu.SemaphoreType.DMA((2, column)),
        ],
        compiler_params=pltpu.CompilerParams(collective_id=0, has_side_effects=True, vmem_limit_bytes=GRANT),
        name="gather",
    )(hamiltonian, self_energy, guess_factor, weights, counts)


def newton_kernel(f_ref, rows, counts_ref, left_ref, right_ref, work, counts):
    column, slots, pairs, _, orbitals, width = f_ref.shape
    total_pairs = slots * pairs
    shape = (orbitals, width)
    parity = lax.rem(lax.axis_index("kgrp"), 2)
    branch = lax.rem(lax.axis_index("freq"), 2)
    steps = counts_ref[...]
    step_lane = lax.broadcasted_iota(jnp.int32, steps.shape, 1)
    for index in range(column):
        counts[index] = jnp.sum(jnp.where(step_lane == 2 * (2 * index + branch) + parity, steps, 0))
    row = lax.broadcasted_iota(jnp.int32, shape, 0)
    lane = lax.broadcasted_iota(jnp.int32, shape, 1)
    left = lane < orbitals
    eye_both = (lax.rem(lane, orbitals) == row).astype(jnp.float32)
    eye_half = eye_both.astype(jnp.bfloat16)
    left_half = left.astype(jnp.float32).astype(jnp.bfloat16)
    right_half = (1.0 - left.astype(jnp.float32)).astype(jnp.bfloat16)

    def turn(value):
        return pltpu.roll(value, orbitals, 1)

    def spread(real, imag):
        real_left, real_right = real * left_half, real * right_half
        imag_left, imag_right = imag * left_half, imag * right_half
        return grid_of(
            [
                [real_left, imag_left],
                [real_right, imag_right],
                [-imag_left, real_left],
                [-imag_right, real_right],
            ]
        )

    def parts(real, imag):
        (real_high, real_low), (imag_high, imag_low) = halves(real), halves(imag)
        return (real_high, imag_high), (real_low, imag_low)

    def multiply(highs, lows, right_high, right_low):
        count = len(highs) * orbitals
        high = jnp.concatenate(highs, 0)
        both = dot(jnp.concatenate([high] + lows, 0), spread(*right_high))
        return both[:count] + both[count:] + dot(high, spread(*right_low))

    def beside(pair):
        return jnp.concatenate(pair, 1)

    def one_frequency(index, carry):
        count = counts[index]

        def load_f(p):
            return f_ref[index, p // pairs, p % pairs, 0], f_ref[index, p // pairs, p % pairs, 1]

        lines = []
        for slot in range(slots):
            line = rows[index, slot]
            lines += [line, turn(line)]
        lines.append(jnp.zeros((width - 4 * pairs * slots, width), jnp.float32))
        flat = jnp.transpose(jnp.concatenate(lines, 0))[:orbitals]

        def column_of(at):
            return jnp.take_along_axis(flat, jnp.where(left, at, at + 2 * pairs), axis=1)

        def scaled(p, real, imag):
            first = (p // pairs) * 4 * pairs + p % pairs
            d_real, d_imag = column_of(first), column_of(first + pairs)
            return real * d_real - imag * d_imag, real * d_imag + imag * d_real

        def squares(p):
            real, imag = load_f(p)
            high, low = parts(real, imag)
            product = multiply([beside(high)], [beside(low)], high, low)
            work[p, 0] = product[:, :width]
            work[p, 1] = product[:, width:]

        def cubes(p):
            real, imag = load_f(p)
            square_real, square_imag = work[p, 0], work[p, 1]
            high, low = parts(real, imag)
            square_high, square_low = parts(square_real, square_imag)
            product = multiply(
                [beside(high), beside(square_high)],
                [beside(low), beside(square_low)],
                square_high,
                square_low,
            )
            work[p, 2] = eye_both + real + square_real + product[:orbitals, :width]
            work[p, 3] = imag + square_imag + product[:orbitals, width:]
            work[p, 4] = product[orbitals:, :width]
            work[p, 5] = product[orbitals:, width:]

        def store_left(p, high, low):
            left_ref[index, :orbitals, 2 * p * width : 2 * (p + 1) * width] = beside(high)
            left_ref[index, orbitals:, 2 * p * width : 2 * (p + 1) * width] = beside(low)

        def store_right(p, real, imag):
            lines = []
            for r, i in parts(eye_both + real, imag):
                r_turned, i_turned = turn(r), turn(i)
                lines.append(
                    [
                        r * left_half + i_turned * right_half,
                        r_turned * left_half + i * right_half,
                        r_turned * right_half - i * left_half,
                        r * right_half - i_turned * left_half,
                    ]
                )
            right_ref[index, 2 * p * width : 2 * (p + 1) * width, :] = grid_of(list(zip(*lines)))

        def finish(p, outer, inner):
            store_left(p, *parts(*scaled(p, *outer)))
            store_right(p, *inner)

        @pl.when(count == 1)
        def _():
            for p in range(total_pairs):
                slot, c = p // pairs, p % pairs
                store_left(
                    p,
                    *[
                        [eye_half * line[at : at + 1, :] for at in (c, pairs + c)]
                        for line in halves(rows[index, slot])
                    ],
                )
                store_right(p, *load_f(p))

        @pl.when(count == 2)
        def _():
            for step in range(total_pairs + LAG):
                if step < total_pairs:
                    squares(step)
                if step >= LAG:
                    p = step - LAG
                    real, imag = load_f(p)
                    finish(p, (eye_both + real, imag), (work[p, 0], work[p, 1]))

        @pl.when(count > 2)
        def _():
            for step in range(total_pairs + 2 * LAG):
                if step < total_pairs:
                    squares(step)
                if LAG <= step < total_pairs + LAG:
                    cubes(step - LAG)
                if step >= 2 * LAG:
                    p = step - 2 * LAG
                    finish(p, (work[p, 2], work[p, 3]), (work[p, 4], work[p, 5]))

        return carry

    lax.fori_loop(0, column, one_frequency, 0)


def newton(f_values, rows, counts):
    column, slots, pairs, _, orbitals, width = f_values.shape
    depth = 2 * slots * pairs * width
    return pl.pallas_call(
        newton_kernel,
        out_shape=(
            jax.ShapeDtypeStruct((column, 2 * orbitals, depth), jnp.bfloat16),
            jax.ShapeDtypeStruct((column, depth, 2 * width), jnp.bfloat16),
        ),
        in_specs=[VMEM] * 3,
        out_specs=(VMEM, VMEM),
        scratch_shapes=[
            pltpu.VMEM((slots * pairs, 6, orbitals, width), jnp.float32),
            pltpu.SMEM((column,), jnp.int32),
        ],
        compiler_params=pltpu.CompilerParams(vmem_limit_bytes=GRANT),
        name="newton",
    )(f_values, rows, counts)


def scatter_kernel(left_ref, right_ref, sg_ref, weights_hbm, out_ref, weights, part, landed, load_sem, send, recv):
    freq_devs = lax.axis_size("freq")
    group_devs = lax.axis_size("kgrp")
    column, _, orbitals, width = sg_ref.shape
    tile = landed.shape[2]
    me = lax.axis_index("freq")
    group = lax.axis_index("kgrp")
    others = [(a, b) for a in range(freq_devs) for b in range(group_devs) if a + b > 0]
    barrier = pltpu.get_barrier_semaphore()

    def place(step):
        return lax.rem(me + step[0], freq_devs), lax.rem(group + step[1], group_devs)

    for step in others:
        pl.semaphore_signal(barrier, inc=1, device_id=place(step), device_id_type=MESH)
    load = pltpu.make_async_copy(weights_hbm, weights, load_sem.at[0])
    load.start()

    def spread(index):
        freq_to, group_to = place(others[index])
        return pltpu.make_async_remote_copy(
            src_ref=part.at[pl.ds((freq_to * group_devs + group_to) * tile, tile)],
            dst_ref=landed.at[me, group],
            send_sem=send.at[index],
            recv_sem=recv.at[index],
            device_id=(freq_to, group_to),
            device_id_type=MESH,
        )

    wide_left = lax.broadcasted_iota(jnp.int32, (orbitals, width), 1) < orbitals
    depth = left_ref.shape[2]
    step = 2 * width
    products = []
    for first in range(0, column, 2):
        sums = [None, None]
        for at in range(0, depth, step):
            for offset in range(2):
                index = first + offset
                term = dot(left_ref[index, :, at : at + step], right_ref[index, at : at + step, :])
                sums[offset] = term if at == 0 else sums[offset] + term
        products += sums
    for index in range(column):
        guess = sg_ref[index, 1]
        turned = pltpu.roll(guess, orbitals, 1)
        top = jnp.concatenate(halves(guess), 1)
        bottom = jnp.concatenate(halves(jnp.where(wide_left, -turned, turned)), 1)
        product = products[index]
        total = joined(product[:orbitals]) + product[orbitals:, :width]
        left_side = jnp.concatenate(halves(total), 1)
        green = joined(dot(left_side, jnp.concatenate([top, bottom, top, bottom], 0)))
        part[pl.ds(index, orbitals, stride=column), :] = green
    pl.semaphore_wait(barrier, len(others))
    for index in range(len(others)):
        spread(index).start()
    landed[me, group] = part[pl.ds((me * group_devs + group) * tile, tile), :]
    load.wait()
    total = jnp.sum(weights[...].astype(jnp.float32), axis=0, keepdims=True)
    scale = 1.0 / jnp.broadcast_to(jnp.sum(total, axis=1, keepdims=True), (tile, width))
    for index in range(len(others)):
        spread(index).wait_recv()
    left = lax.broadcasted_iota(jnp.int32, (tile, width), 1) < orbitals
    freq_total = 4 * column
    for branch in range(2):
        for parity in range(2):
            total = None
            for place_at in range(column):
                for high in range(group_devs // 2):
                    term = landed[2 * place_at + branch, 2 * high + parity]
                    total = term if total is None else total + term
            total = total * scale
            swapped = pltpu.roll(total, tile // 2, 0)
            turned = pltpu.roll(total, orbitals, 1)
            turned_swapped = pltpu.roll(turned, tile // 2, 0)
            real = jnp.where(left, total, turned_swapped)
            imag = jnp.where(left, turned, swapped)
            first = 2 * branch + parity
            out_ref[pl.ds(first, column, stride=4), :] = real[:column]
            out_ref[pl.ds(freq_total + first, column, stride=4), :] = imag[:column]
    for index in range(len(others)):
        spread(index).wait_send()


def scatter(left, right, sigma_guess, weights, freq_devs, group_devs):
    column, _, orbitals, width = sigma_guess.shape
    tile = column * orbitals // (freq_devs * group_devs)
    peers = freq_devs * group_devs - 1
    return pl.pallas_call(
        scatter_kernel,
        out_shape=jax.ShapeDtypeStruct((8 * column, width), jnp.float32),
        in_specs=[VMEM, VMEM, VMEM, HBM],
        out_specs=VMEM,
        scratch_shapes=[
            pltpu.VMEM(weights.shape, jnp.int32),
            pltpu.VMEM((column * orbitals, width), jnp.float32),
            pltpu.VMEM((freq_devs, group_devs, tile, width), jnp.float32),
            pltpu.SemaphoreType.DMA((1,)),
            pltpu.SemaphoreType.DMA((peers,)),
            pltpu.SemaphoreType.DMA((peers,)),
        ],
        compiler_params=pltpu.CompilerParams(collective_id=1, has_side_effects=True, vmem_limit_bytes=GRANT),
        name="scatter",
    )(left, right, sigma_guess, weights)


def per_device(hamiltonian, self_energy, guess_factor, weights, counts):
    k_local, orbitals, width = hamiltonian.shape
    per_freq = self_energy.shape[0]
    freq_devs = lax.axis_size("freq")
    group_devs = lax.axis_size("kgrp")
    freq_total = per_freq * freq_devs
    pair_block = orbitals * orbitals // (freq_devs * group_devs)
    column = freq_devs // 2
    direct = (
        width == 128
        and per_freq == 2
        and freq_devs % 2 == 0
        and group_devs % 2 == 0
        and pair_block == width
        and column == 4
        and k_local == 8
        and weights.shape[0] % width == 0
    )
    if direct:
        table = weights.reshape(-1, width)
        inputs = [
            pltpu.with_memory_space_constraint(value, pltpu.HBM)
            for value in (hamiltonian, self_energy, guess_factor, table, counts.reshape(1, -1))
        ]
        values, rows, sigma_guess, steps = gather(*inputs, column)
        left, right = newton(values, rows, steps)
        return scatter(left, right, sigma_guess, inputs[3], freq_devs, group_devs).T
    sigma = lax.all_gather(self_energy, "freq", axis=0, tiled=True)
    guess = lax.all_gather(guess_factor, "freq", axis=0, tiled=True)
    current, factors = early_steps(counts, weights, hamiltonian, sigma, guess)
    terms = local_sum(factors, hamiltonian, sigma, current)
    terms = terms.reshape(freq_total, orbitals, 2, orbitals).transpose(1, 3, 2, 0)
    terms = terms.reshape(orbitals * orbitals, 2 * freq_total)
    result = lax.psum_scatter(terms, ("freq", "kgrp"), scatter_dimension=0, tiled=True)
    return result.reshape(pair_block, 2 * freq_total)


def solution(mesh):
    return jax.shard_map(
        per_device,
        mesh=mesh,
        in_specs=(
            P(("freq", "kgrp"), None, None),
            P("freq", None, None),
            P("freq", None, None),
            P(),
            P(),
        ),
        out_specs=P(("freq", "kgrp"), None),
        check_vma=False,
    )
```

```python
import functools
import math

import jax
import jax.numpy as jnp
from jax import lax
from jax.experimental import pallas as pl
from jax.experimental.pallas import tpu as pltpu
from jax.sharding import PartitionSpec as P

chem_potential = 0.2
MESH = pl.DeviceIdType.MESH
GRANT = 32 * 1024 * 1024
VMEM = pl.BlockSpec(memory_space=pltpu.VMEM)
SMEM = pl.BlockSpec(memory_space=pltpu.SMEM)
HBM = pl.BlockSpec(memory_space=pltpu.HBM)
LAG = 4
TAIL = 4


def split(value):
    high = value.astype(jnp.bfloat16).astype(jnp.float32)
    return high, value - high


def left_operand(value, half, left):
    high, low = split(value)
    turned_high, turned_low = split(pltpu.roll(value, half, 1))
    top = jnp.where(left, high, turned_low)
    bottom = jnp.where(left, turned_high, low)
    return jnp.concatenate([top, bottom], 0).astype(jnp.bfloat16)


def right_operand(value):
    high, low = split(value)
    row = jnp.concatenate([high, low], 1).astype(jnp.bfloat16)
    return jnp.concatenate([row, row], 0)


def fold(product, orbitals, sign):
    width = 2 * orbitals
    both = product[:, :width] + product[:, width:]
    return both[:orbitals] + sign * pltpu.roll(both[orbitals:], orbitals, 1)


def masks(shape):
    orbitals = shape[0]
    row = lax.broadcasted_iota(jnp.int32, shape, 0)
    lane = lax.broadcasted_iota(jnp.int32, shape, 1)
    left = lane < orbitals
    sign = jnp.where(left, -1.0, 1.0)
    eye_real = (lane == row).astype(jnp.float32)
    eye_imag = (lane == row + orbitals).astype(jnp.float32)
    return left, sign, eye_real, eye_imag


def shifted(freq, freq_total, eye_real, eye_imag, sigma):
    matsubara = (2 * freq + 1).astype(jnp.float32) * (math.pi / (2 * freq_total))
    return (chem_potential * eye_real + matsubara * eye_imag) - sigma


def steps_kernel(counts, weights, h_ref, sigma_ref, guess_ref, x_ref, factor_ref, m_left, h_diag):
    k_local, orbitals, width = h_ref.shape
    freq_total = sigma_ref.shape[0]
    shape = (orbitals, width)
    left, sign, eye_real, eye_imag = masks(shape)
    device = lax.axis_index("freq") * lax.axis_size("kgrp") + lax.axis_index("kgrp")

    def add_weight(index, total):
        return total + weights[index]

    weight_total = lax.fori_loop(
        0, weights.shape[0], add_weight, jnp.int32(0), unroll=8
    ).astype(jnp.float32)
    for k in range(k_local):
        weight = weights[device * k_local + k].astype(jnp.float32)
        factor_ref[k : k + 1, :] = jnp.full((1, width), weight) / weight_total

    def diagonal(value):
        real = jnp.sum(value * eye_real, axis=1, keepdims=True)
        imag = jnp.sum(value * eye_imag, axis=1, keepdims=True)
        return jnp.broadcast_to(real, shape), jnp.broadcast_to(imag, shape)

    for k in range(k_local):
        h_diag[0, k], h_diag[1, k] = diagonal(h_ref[k])

    def one_frequency(freq, carry):
        base = shifted(freq, freq_total, eye_real, eye_imag, sigma_ref[freq])
        base_real, base_imag = diagonal(base)
        guess = guess_ref[freq]
        turned = sign * pltpu.roll(guess, orbitals, 1)
        for k in range(k_local):
            real = base_real - h_diag[0, k]
            imag = base_imag - h_diag[1, k]
            inverse = 1.0 / (real * real + imag * imag)
            x_ref[freq, k] = (real * inverse) * guess - (imag * inverse) * turned

        @pl.when(counts[freq] > 1)
        def _():
            for k in range(k_local):
                m_left[k] = left_operand(base - h_ref[k], orbitals, left)

            def newton_step(sweep, inner):
                products = [
                    jnp.dot(
                        m_left[k],
                        right_operand(x_ref[freq, k]),
                        preferred_element_type=jnp.float32,
                    )
                    for k in range(k_local)
                ]
                products = [
                    jnp.dot(
                        left_operand(x_ref[freq, k], orbitals, left),
                        right_operand(eye_real - fold(products[k], orbitals, sign)),
                        preferred_element_type=jnp.float32,
                    )
                    for k in range(k_local)
                ]
                for k in range(k_local):
                    x_ref[freq, k] = x_ref[freq, k] + fold(products[k], orbitals, sign)
                return inner

            lax.fori_loop(0, counts[freq] - 1, newton_step, 0)

        return carry

    lax.fori_loop(0, freq_total, one_frequency, 0)


def early_steps(counts, weights, hamiltonian, sigma, guess):
    k_local, orbitals, width = hamiltonian.shape
    freq_total = sigma.shape[0]
    return pl.pallas_call(
        steps_kernel,
        out_shape=(
            jax.ShapeDtypeStruct((freq_total, k_local, orbitals, width), jnp.float32),
            jax.ShapeDtypeStruct((k_local, width), jnp.float32),
        ),
        in_specs=[SMEM, SMEM, VMEM, VMEM, VMEM],
        out_specs=(VMEM, VMEM),
        scratch_shapes=[
            pltpu.VMEM((k_local, width, width), jnp.bfloat16),
            pltpu.VMEM((2, k_local, orbitals, width), jnp.float32),
        ],
        compiler_params=pltpu.CompilerParams(vmem_limit_bytes=GRANT),
        name="early_steps",
    )(counts, weights, hamiltonian, sigma, guess)


def last_step(freq, freq_total, factor_ref, h_ref, sigma_ref, x_ref, last_left, last_right):
    k_local, orbitals, width = h_ref.shape
    left, sign, eye_real, eye_imag = masks((orbitals, width))
    base = shifted(freq, freq_total, eye_real, eye_imag, sigma_ref[freq])
    products = [
        jnp.dot(
            left_operand(base - h_ref[k], orbitals, left),
            right_operand(x_ref[freq, k]),
            preferred_element_type=jnp.float32,
        )
        for k in range(k_local)
    ]
    total = jnp.zeros((orbitals, width), jnp.float32)
    for k in range(k_local):
        weighted = x_ref[freq, k] * factor_ref[k : k + 1, :]
        last_left[:, k * width : (k + 1) * width] = left_operand(weighted, orbitals, left)
        total = total + weighted
    for k in range(k_local):
        missing = eye_real - fold(products[k], orbitals, sign)
        last_right[k * width : (k + 1) * width, :] = right_operand(missing)
    product = jnp.dot(last_left[...], last_right[...], preferred_element_type=jnp.float32)
    return total + fold(product, orbitals, sign)


def last_scratch(k_local, width):
    return [
        pltpu.VMEM((width, k_local * width), jnp.bfloat16),
        pltpu.VMEM((k_local * width, 2 * width), jnp.bfloat16),
    ]


def sum_kernel(factor_ref, h_ref, sigma_ref, x_ref, out_ref, last_left, last_right):
    freq_total = sigma_ref.shape[0]

    def one_frequency(freq, carry):
        out_ref[freq] = last_step(
            freq, freq_total, factor_ref, h_ref, sigma_ref, x_ref, last_left, last_right
        )
        return carry

    lax.fori_loop(0, freq_total, one_frequency, 0)


def local_sum(factors, hamiltonian, sigma, current):
    k_local, orbitals, width = hamiltonian.shape
    return pl.pallas_call(
        sum_kernel,
        out_shape=jax.ShapeDtypeStruct(sigma.shape, jnp.float32),
        in_specs=[VMEM] * 4,
        out_specs=VMEM,
        scratch_shapes=last_scratch(k_local, width),
        name="local_sum",
    )(factors, hamiltonian, sigma, current)


def halves(value):
    high = value.astype(jnp.bfloat16)
    return high, (value - high.astype(jnp.float32)).astype(jnp.bfloat16)


def joined(product):
    width = product.shape[1] // 2
    return product[:, :width] + product[:, width:]


def dot(left_side, right_side):
    return jnp.dot(left_side, right_side, preferred_element_type=jnp.float32)


def grid_of(blocks):
    return jnp.concatenate([jnp.concatenate(line, 1) for line in blocks], 0)


def gather_kernel(
    h_hbm,
    sigma_hbm,
    guess_hbm,
    weights_hbm,
    counts_hbm,
    f_out,
    rows_out,
    sg_out,
    counts_out,
    own_h,
    packed,
    weights,
    right_ref,
    g_side,
    g_shift,
    shift_rows,
    h_rows,
    scales,
    local,
    mate_sem,
    pair_sem,
    pass_sem,
    col_sem,
):
    column, slots, pairs, _, orbitals, width = f_out.shape
    k_local = 2 * pairs
    shape = (orbitals, width)
    freq_devs = 2 * column
    freq_total = 2 * freq_devs
    me = lax.axis_index("freq")
    group = lax.axis_index("kgrp")
    group_devs = lax.axis_size("kgrp")
    parity = lax.rem(group, 2)
    branch = lax.rem(me, 2)
    place = me // 2
    pair = me + 1 - 2 * branch
    mate = group + 1 - 2 * parity
    others = [place + 1 - 2 * lax.rem(place, 2), lax.rem(place + 2, column), column - 1 - place]
    barrier = pltpu.get_barrier_semaphore()
    for other in others:
        pl.semaphore_signal(barrier, inc=1, device_id=(2 * other + branch, group), device_id_type=MESH)
    pl.semaphore_signal(barrier, inc=1, device_id=(pair, group), device_id_type=MESH)
    pl.semaphore_signal(barrier, inc=1, device_id=(me, mate), device_id_type=MESH)
    loads = [
        pltpu.make_async_copy(h_hbm, own_h, local.at[0]),
        pltpu.make_async_copy(sigma_hbm.at[parity], sg_out.at[place, 0], local.at[1]),
        pltpu.make_async_copy(guess_hbm.at[parity], sg_out.at[place, 1], local.at[2]),
        pltpu.make_async_copy(weights_hbm, weights, local.at[3]),
        pltpu.make_async_copy(counts_hbm, counts_out, local.at[4]),
    ]
    for load in loads:
        load.start()

    def remote(src, dst, sems, slot, freq_to, group_to):
        return pltpu.make_async_remote_copy(
            src_ref=src,
            dst_ref=dst,
            send_sem=sems.at[0, slot],
            recv_sem=sems.at[1, slot],
            device_id=(freq_to, group_to),
            device_id_type=MESH,
        )

    own = sg_out.at[place]
    columns = [
        remote(own, own, col_sem, index, 2 * others[index] + branch, group) for index in range(column - 1)
    ]
    across = [remote(packed.at[0, c], packed.at[2, c], pair_sem, c, pair, group) for c in range(pairs)]
    passes = [remote(packed.at[2, c], packed.at[3, c], pass_sem, c, me, mate) for c in range(pairs)]
    beside = remote(packed.at[0], packed.at[1], mate_sem, 0, me, mate)

    row = lax.broadcasted_iota(jnp.int32, shape, 0)
    lane = lax.broadcasted_iota(jnp.int32, shape, 1)
    left = lane < orbitals
    within = jnp.where(left, lane, lane - orbitals)
    upper = within >= row
    above = within > row
    eye_both = (within == row).astype(jnp.float32)

    def turn(value):
        return pltpu.roll(value, orbitals, 1)

    def planes(slot, c, real, imag):
        diagonal = jnp.sum(eye_both * real, axis=0, keepdims=True)
        h_rows[slot, c : c + 1, :] = diagonal
        h_rows[slot, pairs + c : pairs + c + 1, :] = diagonal
        for part, (r, i) in enumerate(zip(halves(real), halves(imag))):
            right_ref[slot, c, part] = grid_of([[r, i], [-i, r]])

    loads[0].wait()
    for c in range(pairs):
        one, two = own_h[2 * c], own_h[2 * c + 1]
        real = jnp.where(left, one, turn(two))
        imag = jnp.where(left, turn(one), two)
        packed[0, c] = jnp.where(upper, real, imag)
    loads[1].wait()
    loads[2].wait()
    pl.semaphore_wait(barrier, column + 1)
    for copy in across + columns + [beside]:
        copy.start()
    loads[3].wait()
    loads[4].wait()

    def times(guess_side, right_high, right_low):
        return dot(guess_side, jnp.concatenate([right_high, right_high, right_low], 0))

    def prepare(index):
        frequency = 2 * (2 * index + branch) + parity
        matsubara = (2 * frequency + 1).astype(jnp.float32) * (math.pi / (2 * freq_total))
        sigma = sg_out[index, 0]
        swapped = turn(sigma)
        real = chem_potential * eye_both - jnp.where(left, sigma, swapped)
        imag = matsubara * eye_both - jnp.where(left, swapped, sigma)
        high, low = halves(sg_out[index, 1])
        guess_side = jnp.concatenate([high, low, high], 1)
        g_side[index] = guess_side
        shift_rows[index, 0] = jnp.broadcast_to(jnp.sum(eye_both * real, axis=0, keepdims=True), tile)
        shift_rows[index, 1] = jnp.broadcast_to(jnp.sum(eye_both * imag, axis=0, keepdims=True), tile)
        (real_high, real_low), (imag_high, imag_low) = halves(real), halves(imag)
        product = times(
            guess_side,
            grid_of([[real_high, imag_high], [-imag_high, real_high]]),
            grid_of([[real_low, imag_low], [-imag_low, real_low]]),
        )
        g_shift[index] = product

    def unpack(slot):
        for c in range(pairs):
            value = packed[slot, c]
            flipped = jnp.transpose(value)
            other = jnp.concatenate([flipped[:orbitals], flipped[orbitals:]], 1)
            real = jnp.where(upper, value, other)
            imag = jnp.where(above, -other, jnp.where(upper, 0.0, value))
            planes(slot, c, real, imag)

    tile = (2 * pairs, width)
    tile_row = lax.broadcasted_iota(jnp.int32, tile, 0)
    tile_left = lax.broadcasted_iota(jnp.int32, tile, 1) < orbitals
    tile_real = tile_row < pairs
    tile_k = 2 * jnp.where(tile_real, tile_row, tile_row - pairs) + jnp.where(tile_left, 0, 1)

    def slot_weights(slot):
        owner_freq = me + (slot // 2) * (1 - 2 * branch)
        owner_group = group + (slot % 2) * (1 - 2 * parity)
        k_first = (owner_freq * group_devs + owner_group) * k_local
        first_row, first_column = lax.div(k_first, width), lax.rem(k_first, width)
        weight = jnp.zeros(tile, jnp.float32)
        for j in range(k_local):
            value = weights[first_row, first_column + j].astype(jnp.float32)
            weight = jnp.where(tile_k == j, value, weight)
        return weight

    def apply(at_slots, indices):
        for slot in at_slots:
            weight = slot_weights(slot)
            for index in indices:
                real = shift_rows[index, 0] - h_rows[slot]
                imag = shift_rows[index, 1]
                inverse = 1.0 / (real * real + imag * imag)
                scale = jnp.where(tile_real, real * inverse, -imag * inverse)
                scales[index, slot] = scale
                rows_out[index, slot] = weight * scale
        side = jnp.concatenate([g_side[index] for index in indices], 0)
        for slot in at_slots:
            for c in range(pairs):
                product = times(side, right_ref[slot, c, 0], right_ref[slot, c, 1])
                for at, index in enumerate(indices):
                    q = g_shift[index] - product[at * orbitals : (at + 1) * orbitals]
                    d_real = scales[index, slot, c : c + 1, :]
                    d_imag = scales[index, slot, pairs + c : pairs + c + 1, :]
                    real, imag = q[:, :width], q[:, width:]
                    f_out[index, slot, c, 0] = eye_both - real * d_real + imag * d_imag
                    f_out[index, slot, c, 1] = -real * d_imag - imag * d_real

    prepare(place)
    unpack(0)
    beside.wait_recv()
    unpack(1)
    columns[0].wait_recv()
    prepare(others[0])
    apply([0, 1], [place, others[0]])
    for c in range(pairs):
        across[c].wait_recv()
        passes[c].start()
    unpack(2)
    apply([2], [place, others[0]])
    for copy in passes:
        copy.wait_recv()
    unpack(3)
    apply([3], [place, others[0]])
    for index in range(1, column - 1):
        columns[index].wait_recv()
        prepare(others[index])
    apply(range(slots), others[1:])
    for copy in columns + across + passes + [beside]:
        copy.wait_send()


def gather(hamiltonian, self_energy, guess_factor, weights, counts, column):
    k_local, orbitals, width = hamiltonian.shape
    pairs = k_local // 2
    return pl.pallas_call(
        gather_kernel,
        out_shape=(
            jax.ShapeDtypeStruct((column, 4, pairs, 2, orbitals, width), jnp.float32),
            jax.ShapeDtypeStruct((column, 4, k_local, width), jnp.float32),
            jax.ShapeDtypeStruct((column, 2, orbitals, width), jnp.float32),
            jax.ShapeDtypeStruct(counts.shape, jnp.int32),
        ),
        in_specs=[HBM] * 5,
        out_specs=(VMEM,) * 4,
        scratch_shapes=[
            pltpu.VMEM((k_local, orbitals, width), jnp.float32),
            pltpu.VMEM((4, pairs, orbitals, width), jnp.float32),
            pltpu.SMEM(weights.shape, jnp.int32),
            pltpu.VMEM((4, pairs, 2, width, 2 * width), jnp.bfloat16),
            pltpu.VMEM((column, orbitals, 3 * width), jnp.bfloat16),
            pltpu.VMEM((column, orbitals, 2 * width), jnp.float32),
            pltpu.VMEM((column, 2, k_local, width), jnp.float32),
            pltpu.VMEM((4, k_local, width), jnp.float32),
            pltpu.VMEM((column, 4, k_local, width), jnp.float32),
            pltpu.SemaphoreType.DMA((5,)),
            pltpu.SemaphoreType.DMA((2, 1)),
            pltpu.SemaphoreType.DMA((2, pairs)),
            pltpu.SemaphoreType.DMA((2, pairs)),
            pltpu.SemaphoreType.DMA((2, column)),
        ],
        compiler_params=pltpu.CompilerParams(collective_id=0, has_side_effects=True, vmem_limit_bytes=GRANT),
        name="gather",
    )(hamiltonian, self_energy, guess_factor, weights, counts)


class Tools:
    def __init__(self, orbitals, width):
        self.orbitals, self.width = orbitals, width
        shape = (orbitals, width)
        row = lax.broadcasted_iota(jnp.int32, shape, 0)
        lane = lax.broadcasted_iota(jnp.int32, shape, 1)
        self.left = lane < orbitals
        self.eye_both = (lax.rem(lane, orbitals) == row).astype(jnp.float32)
        self.eye_half = self.eye_both.astype(jnp.bfloat16)
        self.left_half = self.left.astype(jnp.float32).astype(jnp.bfloat16)
        self.right_half = (1.0 - self.left.astype(jnp.float32)).astype(jnp.bfloat16)
        self.left_mask = self.left_half > self.right_half

    def turn(self, value):
        return pltpu.roll(value, self.orbitals, 1)

    def columns(self, rows, index):
        slots, lines_each = rows.shape[1], rows.shape[2]
        lines = []
        for slot in range(slots):
            line = rows[index, slot]
            lines += [line, self.turn(line)]
        lines.append(jnp.zeros((self.width - 2 * lines_each * slots, self.width), jnp.float32))
        return jnp.transpose(jnp.concatenate(lines, 0))[: self.orbitals]

    def scaled(self, flat, pairs, p, real, imag):
        def column_of(at):
            return jnp.take_along_axis(flat, jnp.where(self.left, at, at + 2 * pairs), axis=1)

        first = (p // pairs) * 4 * pairs + p % pairs
        d_real, d_imag = column_of(first), column_of(first + pairs)
        return real * d_real - imag * d_imag, real * d_imag + imag * d_real

    def store_left(self, ref, index, at, high, low):
        span = slice(2 * at * self.width, 2 * (at + 1) * self.width)
        ref[index, : self.orbitals, span] = beside(high)
        ref[index, self.orbitals :, span] = beside(low)

    def store_right(self, ref, index, at, real, imag):
        lines = []
        for r, i in parts(self.eye_both + real, imag):
            r_turned, i_turned = self.turn(r), self.turn(i)
            lines.append(
                [
                    jnp.where(self.left_mask, r, i_turned),
                    jnp.where(self.left_mask, r_turned, i),
                    jnp.where(self.left_mask, -i, r_turned),
                    jnp.where(self.left_mask, -i_turned, r),
                ]
            )
        ref[index, 2 * at * self.width : 2 * (at + 1) * self.width, :] = grid_of(list(zip(*lines)))


def parts(real, imag):
    (real_high, real_low), (imag_high, imag_low) = halves(real), halves(imag)
    return (real_high, imag_high), (real_low, imag_low)


def beside(pair):
    return jnp.concatenate(pair, 1)


def newton_kernel(f_ref, rows, counts_ref, left_ref, right_ref, tail_ref, work, sides, counts):
    column, slots, pairs, _, orbitals, width = f_ref.shape
    total_pairs = slots * pairs
    kept = total_pairs - tail_ref.shape[1]
    parity = lax.rem(lax.axis_index("kgrp"), 2)
    branch = lax.rem(lax.axis_index("freq"), 2)
    steps = counts_ref[...]
    step_lane = lax.broadcasted_iota(jnp.int32, steps.shape, 1)
    for index in range(column):
        counts[index] = jnp.sum(jnp.where(step_lane == 2 * (2 * index + branch) + parity, steps, 0))
    tools = Tools(orbitals, width)
    eye_both = tools.eye_both

    def spread(real, imag):
        real_left, real_right = real * tools.left_half, real * tools.right_half
        imag_left, imag_right = imag * tools.left_half, imag * tools.right_half
        return grid_of(
            [
                [real_left, imag_left],
                [real_right, imag_right],
                [-imag_left, real_left],
                [-imag_right, real_right],
            ]
        )

    def multiply(highs, lows, right_high, right_low):
        count = len(highs) * orbitals
        high = jnp.concatenate(highs, 0)
        both = dot(jnp.concatenate([high] + lows, 0), spread(*right_high))
        return both[:count] + both[count:] + dot(high, spread(*right_low))

    def one_frequency(index, carry):
        count = counts[index]

        def load_f(p):
            return f_ref[index, p // pairs, p % pairs, 0], f_ref[index, p // pairs, p % pairs, 1]

        def squares(p):
            real, imag = load_f(p)
            high, low = parts(real, imag)
            sides[p, 0], sides[p, 1] = beside(high), beside(low)
            product = multiply([beside(high)], [beside(low)], high, low)
            work[p, 0] = product[:, :width]
            work[p, 1] = product[:, width:]

        def keep(p, values):
            for at, value in enumerate(values):
                if p >= kept:
                    tail_ref[index, p - kept, at] = value
                else:
                    work[p, 2 + at] = value

        def cubes(p):
            real, imag = load_f(p)
            square_real, square_imag = work[p, 0], work[p, 1]
            square_high, square_low = parts(square_real, square_imag)
            product = multiply(
                [sides[p, 0], beside(square_high)],
                [sides[p, 1], beside(square_low)],
                square_high,
                square_low,
            )
            keep(
                p,
                [
                    eye_both + real + square_real + product[:orbitals, :width],
                    imag + square_imag + product[:orbitals, width:],
                    product[orbitals:, :width],
                    product[orbitals:, width:],
                ],
            )

        def finish(flat, p, outer, inner):
            high, low = parts(*tools.scaled(flat, pairs, p, *outer))
            tools.store_left(left_ref, index, p, high, low)
            tools.store_right(right_ref, index, p, *inner)

        @pl.when(count == 1)
        def _():
            for p in range(total_pairs):
                slot, c = p // pairs, p % pairs
                real, imag = load_f(p)
                if p >= kept:
                    keep(p, [eye_both, jnp.zeros_like(eye_both), real, imag])
                    continue
                high, low = [
                    [tools.eye_half * line[at : at + 1, :] for at in (c, pairs + c)]
                    for line in halves(rows[index, slot])
                ]
                tools.store_left(left_ref, index, p, high, low)
                tools.store_right(right_ref, index, p, real, imag)

        @pl.when(count == 2)
        def _():
            flat = tools.columns(rows, index)
            for step in range(total_pairs + LAG):
                if step < total_pairs:
                    squares(step)
                if step >= LAG:
                    p = step - LAG
                    real, imag = load_f(p)
                    if p >= kept:
                        keep(p, [eye_both + real, imag, work[p, 0], work[p, 1]])
                    else:
                        finish(flat, p, (eye_both + real, imag), (work[p, 0], work[p, 1]))

        @pl.when(count > 2)
        def _():
            flat = tools.columns(rows, index)
            for step in range(total_pairs + 2 * LAG):
                if step < total_pairs:
                    squares(step)
                if LAG <= step < total_pairs + LAG:
                    cubes(step - LAG)
                if 2 * LAG <= step < kept + 2 * LAG:
                    p = step - 2 * LAG
                    finish(flat, p, (work[p, 2], work[p, 3]), (work[p, 4], work[p, 5]))

        return carry

    lax.fori_loop(0, column, one_frequency, 0)


def newton(f_values, rows, counts):
    column, slots, pairs, _, orbitals, width = f_values.shape
    depth = 2 * (slots * pairs - TAIL) * width
    return pl.pallas_call(
        newton_kernel,
        out_shape=(
            jax.ShapeDtypeStruct((column, 2 * orbitals, depth), jnp.bfloat16),
            jax.ShapeDtypeStruct((column, depth, 2 * width), jnp.bfloat16),
            jax.ShapeDtypeStruct((column, TAIL, 4, orbitals, width), jnp.float32),
        ),
        in_specs=[VMEM] * 3,
        out_specs=(VMEM,) * 3,
        scratch_shapes=[
            pltpu.VMEM((slots * pairs, 6, orbitals, width), jnp.float32),
            pltpu.VMEM((slots * pairs, 2, orbitals, 2 * width), jnp.bfloat16),
            pltpu.SMEM((column,), jnp.int32),
        ],
        compiler_params=pltpu.CompilerParams(vmem_limit_bytes=GRANT),
        name="newton",
    )(f_values, rows, counts)


def scatter_kernel(
    left_ref,
    right_ref,
    tail_ref,
    rows,
    sg_ref,
    weights_hbm,
    out_ref,
    weights,
    left_tail,
    right_tail,
    part,
    landed,
    load_sem,
    send,
    recv,
):
    freq_devs = lax.axis_size("freq")
    group_devs = lax.axis_size("kgrp")
    column, _, orbitals, width = sg_ref.shape
    tile = landed.shape[2]
    me = lax.axis_index("freq")
    group = lax.axis_index("kgrp")
    others = [(a, b) for a in range(freq_devs) for b in range(group_devs) if a + b > 0]
    barrier = pltpu.get_barrier_semaphore()

    def place(step):
        return lax.rem(me + step[0], freq_devs), lax.rem(group + step[1], group_devs)

    for step in others:
        pl.semaphore_signal(barrier, inc=1, device_id=place(step), device_id_type=MESH)
    load = pltpu.make_async_copy(weights_hbm, weights, load_sem.at[0])
    load.start()

    def spread(index):
        freq_to, group_to = place(others[index])
        return pltpu.make_async_remote_copy(
            src_ref=part.at[pl.ds((freq_to * group_devs + group_to) * tile, tile)],
            dst_ref=landed.at[me, group],
            send_sem=send.at[index],
            recv_sem=recv.at[index],
            device_id=(freq_to, group_to),
            device_id_type=MESH,
        )

    wide_left = lax.broadcasted_iota(jnp.int32, (orbitals, width), 1) < orbitals
    tools = Tools(orbitals, width)
    pairs = rows.shape[2] // 2
    tail = tail_ref.shape[1]
    kept = rows.shape[1] * pairs - tail
    for index in range(column):
        flat = tools.columns(rows, index)
        for at in range(tail):
            high, low = parts(*tools.scaled(flat, pairs, kept + at, tail_ref[index, at, 0], tail_ref[index, at, 1]))
            tools.store_left(left_tail, index, at, high, low)
            tools.store_right(right_tail, index, at, tail_ref[index, at, 2], tail_ref[index, at, 3])
    step = 2 * width
    chunks = [(left_ref, right_ref, at * step) for at in range(kept)]
    chunks += [(left_tail, right_tail, at * step) for at in range(tail)]
    products = []
    for first in range(0, column, 2):
        sums = [None, None]
        for left_side, right_side, at in chunks:
            for offset in range(2):
                index = first + offset
                term = dot(left_side[index, :, at : at + step], right_side[index, at : at + step, :])
                sums[offset] = term if sums[offset] is None else sums[offset] + term
        products += sums
    for index in range(column):
        guess = sg_ref[index, 1]
        turned = pltpu.roll(guess, orbitals, 1)
        top = jnp.concatenate(halves(guess), 1)
        bottom = jnp.concatenate(halves(jnp.where(wide_left, -turned, turned)), 1)
        product = products[index]
        total = joined(product[:orbitals]) + product[orbitals:, :width]
        left_side = jnp.concatenate(halves(total), 1)
        green = joined(dot(left_side, jnp.concatenate([top, bottom, top, bottom], 0)))
        part[pl.ds(index, orbitals, stride=column), :] = green
    pl.semaphore_wait(barrier, len(others))
    for index in range(len(others)):
        spread(index).start()
    landed[me, group] = part[pl.ds((me * group_devs + group) * tile, tile), :]
    load.wait()
    total = jnp.sum(weights[...].astype(jnp.float32), axis=0, keepdims=True)
    scale = 1.0 / jnp.broadcast_to(jnp.sum(total, axis=1, keepdims=True), (tile, width))
    for index in range(len(others)):
        spread(index).wait_recv()
    left = lax.broadcasted_iota(jnp.int32, (tile, width), 1) < orbitals
    freq_total = 4 * column
    for branch in range(2):
        for parity in range(2):
            total = None
            for place_at in range(column):
                for high in range(group_devs // 2):
                    term = landed[2 * place_at + branch, 2 * high + parity]
                    total = term if total is None else total + term
            total = total * scale
            swapped = pltpu.roll(total, tile // 2, 0)
            turned = pltpu.roll(total, orbitals, 1)
            turned_swapped = pltpu.roll(turned, tile // 2, 0)
            real = jnp.where(left, total, turned_swapped)
            imag = jnp.where(left, turned, swapped)
            first = 2 * branch + parity
            out_ref[pl.ds(first, column, stride=4), :] = real[:column]
            out_ref[pl.ds(freq_total + first, column, stride=4), :] = imag[:column]
    for index in range(len(others)):
        spread(index).wait_send()


def scatter(left, right, rest, rows, sigma_guess, weights, freq_devs, group_devs):
    column, _, orbitals, width = sigma_guess.shape
    tile = column * orbitals // (freq_devs * group_devs)
    peers = freq_devs * group_devs - 1
    return pl.pallas_call(
        scatter_kernel,
        out_shape=jax.ShapeDtypeStruct((8 * column, width), jnp.float32),
        in_specs=[VMEM] * 5 + [HBM],
        out_specs=VMEM,
        scratch_shapes=[
            pltpu.VMEM(weights.shape, jnp.int32),
            pltpu.VMEM((column, 2 * orbitals, 2 * TAIL * width), jnp.bfloat16),
            pltpu.VMEM((column, 2 * TAIL * width, 2 * width), jnp.bfloat16),
            pltpu.VMEM((column * orbitals, width), jnp.float32),
            pltpu.VMEM((freq_devs, group_devs, tile, width), jnp.float32),
            pltpu.SemaphoreType.DMA((1,)),
            pltpu.SemaphoreType.DMA((peers,)),
            pltpu.SemaphoreType.DMA((peers,)),
        ],
        compiler_params=pltpu.CompilerParams(collective_id=1, has_side_effects=True, vmem_limit_bytes=GRANT),
        name="scatter",
    )(left, right, rest, rows, sigma_guess, weights)


def per_device(hamiltonian, self_energy, guess_factor, weights, counts):
    k_local, orbitals, width = hamiltonian.shape
    per_freq = self_energy.shape[0]
    freq_devs = lax.axis_size("freq")
    group_devs = lax.axis_size("kgrp")
    freq_total = per_freq * freq_devs
    pair_block = orbitals * orbitals // (freq_devs * group_devs)
    column = freq_devs // 2
    direct = (
        width == 128
        and per_freq == 2
        and freq_devs % 2 == 0
        and group_devs % 2 == 0
        and pair_block == width
        and column == 4
        and k_local == 8
        and weights.shape[0] % width == 0
    )
    if direct:
        table = weights.reshape(-1, width)
        inputs = [
            pltpu.with_memory_space_constraint(value, pltpu.HBM)
            for value in (hamiltonian, self_energy, guess_factor, table, counts.reshape(1, -1))
        ]
        values, rows, sigma_guess, steps = gather(*inputs, column)
        left, right, rest = newton(values, rows, steps)
        return scatter(left, right, rest, rows, sigma_guess, inputs[3], freq_devs, group_devs).T
    sigma = lax.all_gather(self_energy, "freq", axis=0, tiled=True)
    guess = lax.all_gather(guess_factor, "freq", axis=0, tiled=True)
    current, factors = early_steps(counts, weights, hamiltonian, sigma, guess)
    terms = local_sum(factors, hamiltonian, sigma, current)
    terms = terms.reshape(freq_total, orbitals, 2, orbitals).transpose(1, 3, 2, 0)
    terms = terms.reshape(orbitals * orbitals, 2 * freq_total)
    result = lax.psum_scatter(terms, ("freq", "kgrp"), scatter_dimension=0, tiled=True)
    return result.reshape(pair_block, 2 * freq_total)


def solution(mesh):
    return jax.shard_map(
        per_device,
        mesh=mesh,
        in_specs=(
            P(("freq", "kgrp"), None, None),
            P("freq", None, None),
            P("freq", None, None),
            P(),
            P(),
        ),
        out_specs=P(("freq", "kgrp"), None),
        check_vma=False,
    )
```

```python
import functools
import math

import jax
import jax.numpy as jnp
from jax import lax
from jax.experimental import pallas as pl
from jax.experimental.pallas import tpu as pltpu
from jax.sharding import PartitionSpec as P

chem_potential = 0.2
MESH = pl.DeviceIdType.MESH
GRANT = 32 * 1024 * 1024
VMEM = pl.BlockSpec(memory_space=pltpu.VMEM)
SMEM = pl.BlockSpec(memory_space=pltpu.SMEM)
HBM = pl.BlockSpec(memory_space=pltpu.HBM)
LAG = 4
TAIL = 4


def split(value):
    high = value.astype(jnp.bfloat16).astype(jnp.float32)
    return high, value - high


def left_operand(value, half, left):
    high, low = split(value)
    turned_high, turned_low = split(pltpu.roll(value, half, 1))
    top = jnp.where(left, high, turned_low)
    bottom = jnp.where(left, turned_high, low)
    return jnp.concatenate([top, bottom], 0).astype(jnp.bfloat16)


def right_operand(value):
    high, low = split(value)
    row = jnp.concatenate([high, low], 1).astype(jnp.bfloat16)
    return jnp.concatenate([row, row], 0)


def fold(product, orbitals, sign):
    width = 2 * orbitals
    both = product[:, :width] + product[:, width:]
    return both[:orbitals] + sign * pltpu.roll(both[orbitals:], orbitals, 1)


def masks(shape):
    orbitals = shape[0]
    row = lax.broadcasted_iota(jnp.int32, shape, 0)
    lane = lax.broadcasted_iota(jnp.int32, shape, 1)
    left = lane < orbitals
    sign = jnp.where(left, -1.0, 1.0)
    eye_real = (lane == row).astype(jnp.float32)
    eye_imag = (lane == row + orbitals).astype(jnp.float32)
    return left, sign, eye_real, eye_imag


def shifted(freq, freq_total, eye_real, eye_imag, sigma):
    matsubara = (2 * freq + 1).astype(jnp.float32) * (math.pi / (2 * freq_total))
    return (chem_potential * eye_real + matsubara * eye_imag) - sigma


def steps_kernel(counts, weights, h_ref, sigma_ref, guess_ref, x_ref, factor_ref, m_left, h_diag):
    k_local, orbitals, width = h_ref.shape
    freq_total = sigma_ref.shape[0]
    shape = (orbitals, width)
    left, sign, eye_real, eye_imag = masks(shape)
    device = lax.axis_index("freq") * lax.axis_size("kgrp") + lax.axis_index("kgrp")

    def add_weight(index, total):
        return total + weights[index]

    weight_total = lax.fori_loop(
        0, weights.shape[0], add_weight, jnp.int32(0), unroll=8
    ).astype(jnp.float32)
    for k in range(k_local):
        weight = weights[device * k_local + k].astype(jnp.float32)
        factor_ref[k : k + 1, :] = jnp.full((1, width), weight) / weight_total

    def diagonal(value):
        real = jnp.sum(value * eye_real, axis=1, keepdims=True)
        imag = jnp.sum(value * eye_imag, axis=1, keepdims=True)
        return jnp.broadcast_to(real, shape), jnp.broadcast_to(imag, shape)

    for k in range(k_local):
        h_diag[0, k], h_diag[1, k] = diagonal(h_ref[k])

    def one_frequency(freq, carry):
        base = shifted(freq, freq_total, eye_real, eye_imag, sigma_ref[freq])
        base_real, base_imag = diagonal(base)
        guess = guess_ref[freq]
        turned = sign * pltpu.roll(guess, orbitals, 1)
        for k in range(k_local):
            real = base_real - h_diag[0, k]
            imag = base_imag - h_diag[1, k]
            inverse = 1.0 / (real * real + imag * imag)
            x_ref[freq, k] = (real * inverse) * guess - (imag * inverse) * turned

        @pl.when(counts[freq] > 1)
        def _():
            for k in range(k_local):
                m_left[k] = left_operand(base - h_ref[k], orbitals, left)

            def newton_step(sweep, inner):
                products = [
                    jnp.dot(
                        m_left[k],
                        right_operand(x_ref[freq, k]),
                        preferred_element_type=jnp.float32,
                    )
                    for k in range(k_local)
                ]
                products = [
                    jnp.dot(
                        left_operand(x_ref[freq, k], orbitals, left),
                        right_operand(eye_real - fold(products[k], orbitals, sign)),
                        preferred_element_type=jnp.float32,
                    )
                    for k in range(k_local)
                ]
                for k in range(k_local):
                    x_ref[freq, k] = x_ref[freq, k] + fold(products[k], orbitals, sign)
                return inner

            lax.fori_loop(0, counts[freq] - 1, newton_step, 0)

        return carry

    lax.fori_loop(0, freq_total, one_frequency, 0)


def early_steps(counts, weights, hamiltonian, sigma, guess):
    k_local, orbitals, width = hamiltonian.shape
    freq_total = sigma.shape[0]
    return pl.pallas_call(
        steps_kernel,
        out_shape=(
            jax.ShapeDtypeStruct((freq_total, k_local, orbitals, width), jnp.float32),
            jax.ShapeDtypeStruct((k_local, width), jnp.float32),
        ),
        in_specs=[SMEM, SMEM, VMEM, VMEM, VMEM],
        out_specs=(VMEM, VMEM),
        scratch_shapes=[
            pltpu.VMEM((k_local, width, width), jnp.bfloat16),
            pltpu.VMEM((2, k_local, orbitals, width), jnp.float32),
        ],
        compiler_params=pltpu.CompilerParams(vmem_limit_bytes=GRANT),
        name="early_steps",
    )(counts, weights, hamiltonian, sigma, guess)


def last_step(freq, freq_total, factor_ref, h_ref, sigma_ref, x_ref, last_left, last_right):
    k_local, orbitals, width = h_ref.shape
    left, sign, eye_real, eye_imag = masks((orbitals, width))
    base = shifted(freq, freq_total, eye_real, eye_imag, sigma_ref[freq])
    products = [
        jnp.dot(
            left_operand(base - h_ref[k], orbitals, left),
            right_operand(x_ref[freq, k]),
            preferred_element_type=jnp.float32,
        )
        for k in range(k_local)
    ]
    total = jnp.zeros((orbitals, width), jnp.float32)
    for k in range(k_local):
        weighted = x_ref[freq, k] * factor_ref[k : k + 1, :]
        last_left[:, k * width : (k + 1) * width] = left_operand(weighted, orbitals, left)
        total = total + weighted
    for k in range(k_local):
        missing = eye_real - fold(products[k], orbitals, sign)
        last_right[k * width : (k + 1) * width, :] = right_operand(missing)
    product = jnp.dot(last_left[...], last_right[...], preferred_element_type=jnp.float32)
    return total + fold(product, orbitals, sign)


def last_scratch(k_local, width):
    return [
        pltpu.VMEM((width, k_local * width), jnp.bfloat16),
        pltpu.VMEM((k_local * width, 2 * width), jnp.bfloat16),
    ]


def sum_kernel(factor_ref, h_ref, sigma_ref, x_ref, out_ref, last_left, last_right):
    freq_total = sigma_ref.shape[0]

    def one_frequency(freq, carry):
        out_ref[freq] = last_step(
            freq, freq_total, factor_ref, h_ref, sigma_ref, x_ref, last_left, last_right
        )
        return carry

    lax.fori_loop(0, freq_total, one_frequency, 0)


def local_sum(factors, hamiltonian, sigma, current):
    k_local, orbitals, width = hamiltonian.shape
    return pl.pallas_call(
        sum_kernel,
        out_shape=jax.ShapeDtypeStruct(sigma.shape, jnp.float32),
        in_specs=[VMEM] * 4,
        out_specs=VMEM,
        scratch_shapes=last_scratch(k_local, width),
        name="local_sum",
    )(factors, hamiltonian, sigma, current)


def halves(value):
    high = value.astype(jnp.bfloat16)
    return high, (value - high.astype(jnp.float32)).astype(jnp.bfloat16)


def joined(product):
    width = product.shape[1] // 2
    return product[:, :width] + product[:, width:]


def dot(left_side, right_side):
    return jnp.dot(left_side, right_side, preferred_element_type=jnp.float32)


def grid_of(blocks):
    return jnp.concatenate([jnp.concatenate(line, 1) for line in blocks], 0)


def gather_kernel(
    h_hbm,
    sigma_hbm,
    guess_hbm,
    weights_hbm,
    counts_hbm,
    f_out,
    rows_out,
    sg_out,
    counts_out,
    own_h,
    packed,
    weights,
    right_ref,
    g_side,
    g_shift,
    shift_rows,
    h_rows,
    scales,
    local,
    mate_sem,
    pair_sem,
    pass_sem,
    col_sem,
):
    column, slots, pairs, _, orbitals, width = f_out.shape
    k_local = 2 * pairs
    shape = (orbitals, width)
    freq_devs = 2 * column
    freq_total = 2 * freq_devs
    me = lax.axis_index("freq")
    group = lax.axis_index("kgrp")
    group_devs = lax.axis_size("kgrp")
    parity = lax.rem(group, 2)
    branch = lax.rem(me, 2)
    place = me // 2
    pair = me + 1 - 2 * branch
    mate = group + 1 - 2 * parity
    others = [place + 1 - 2 * lax.rem(place, 2), lax.rem(place + 2, column), column - 1 - place]
    barrier = pltpu.get_barrier_semaphore()
    for other in others:
        pl.semaphore_signal(barrier, inc=1, device_id=(2 * other + branch, group), device_id_type=MESH)
    pl.semaphore_signal(barrier, inc=1, device_id=(pair, group), device_id_type=MESH)
    pl.semaphore_signal(barrier, inc=1, device_id=(me, mate), device_id_type=MESH)
    loads = [
        pltpu.make_async_copy(h_hbm, own_h, local.at[0]),
        pltpu.make_async_copy(sigma_hbm.at[parity], sg_out.at[place, 0], local.at[1]),
        pltpu.make_async_copy(guess_hbm.at[parity], sg_out.at[place, 1], local.at[2]),
        pltpu.make_async_copy(weights_hbm, weights, local.at[3]),
        pltpu.make_async_copy(counts_hbm, counts_out, local.at[4]),
    ]
    for load in loads:
        load.start()

    def remote(src, dst, sems, slot, freq_to, group_to):
        return pltpu.make_async_remote_copy(
            src_ref=src,
            dst_ref=dst,
            send_sem=sems.at[0, slot],
            recv_sem=sems.at[1, slot],
            device_id=(freq_to, group_to),
            device_id_type=MESH,
        )

    own = sg_out.at[place]
    columns = [
        remote(own, own, col_sem, index, 2 * others[index] + branch, group) for index in range(column - 1)
    ]
    across = [remote(packed.at[0, c], packed.at[2, c], pair_sem, c, pair, group) for c in range(pairs)]
    passes = [remote(packed.at[2, c], packed.at[3, c], pass_sem, c, me, mate) for c in range(pairs)]
    beside = remote(packed.at[0], packed.at[1], mate_sem, 0, me, mate)

    row = lax.broadcasted_iota(jnp.int32, shape, 0)
    lane = lax.broadcasted_iota(jnp.int32, shape, 1)
    left = lane < orbitals
    within = jnp.where(left, lane, lane - orbitals)
    upper = within >= row
    above = within > row
    eye_both = (within == row).astype(jnp.float32)

    def turn(value):
        return pltpu.roll(value, orbitals, 1)

    def planes(slot, c, real, imag):
        diagonal = jnp.sum(eye_both * real, axis=0, keepdims=True)
        h_rows[slot, c : c + 1, :] = diagonal
        h_rows[slot, pairs + c : pairs + c + 1, :] = diagonal
        for part, (r, i) in enumerate(zip(halves(real), halves(imag))):
            right_ref[slot, c, part] = grid_of([[r, i], [-i, r]])

    loads[0].wait()
    for c in range(pairs):
        one, two = own_h[2 * c], own_h[2 * c + 1]
        real = jnp.where(left, one, turn(two))
        imag = jnp.where(left, turn(one), two)
        packed[0, c] = jnp.where(upper, real, imag)
    loads[1].wait()
    loads[2].wait()
    pl.semaphore_wait(barrier, column + 1)
    for copy in columns + across + [beside]:
        copy.start()
    loads[3].wait()
    loads[4].wait()

    def times(guess_side, right_high, right_low):
        return dot(guess_side, jnp.concatenate([right_high, right_high, right_low], 0))

    def prepare(index):
        frequency = 2 * (2 * index + branch) + parity
        matsubara = (2 * frequency + 1).astype(jnp.float32) * (math.pi / (2 * freq_total))
        sigma = sg_out[index, 0]
        swapped = turn(sigma)
        real = chem_potential * eye_both - jnp.where(left, sigma, swapped)
        imag = matsubara * eye_both - jnp.where(left, swapped, sigma)
        high, low = halves(sg_out[index, 1])
        guess_side = jnp.concatenate([high, low, high], 1)
        g_side[index] = guess_side
        shift_rows[index, 0] = jnp.broadcast_to(jnp.sum(eye_both * real, axis=0, keepdims=True), tile)
        shift_rows[index, 1] = jnp.broadcast_to(jnp.sum(eye_both * imag, axis=0, keepdims=True), tile)
        (real_high, real_low), (imag_high, imag_low) = halves(real), halves(imag)
        product = times(
            guess_side,
            grid_of([[real_high, imag_high], [-imag_high, real_high]]),
            grid_of([[real_low, imag_low], [-imag_low, real_low]]),
        )
        g_shift[index] = product

    def unpack(slot):
        for c in range(pairs):
            value = packed[slot, c]
            flipped = jnp.transpose(value)
            other = jnp.concatenate([flipped[:orbitals], flipped[orbitals:]], 1)
            real = jnp.where(upper, value, other)
            imag = jnp.where(above, -other, jnp.where(upper, 0.0, value))
            planes(slot, c, real, imag)

    tile = (2 * pairs, width)
    tile_row = lax.broadcasted_iota(jnp.int32, tile, 0)
    tile_left = lax.broadcasted_iota(jnp.int32, tile, 1) < orbitals
    tile_real = tile_row < pairs
    tile_k = 2 * jnp.where(tile_real, tile_row, tile_row - pairs) + jnp.where(tile_left, 0, 1)

    def slot_weights(slot):
        owner_freq = me + (slot // 2) * (1 - 2 * branch)
        owner_group = group + (slot % 2) * (1 - 2 * parity)
        k_first = (owner_freq * group_devs + owner_group) * k_local
        first_row, first_column = lax.div(k_first, width), lax.rem(k_first, width)
        weight = jnp.zeros(tile, jnp.float32)
        for j in range(k_local):
            value = weights[first_row, first_column + j].astype(jnp.float32)
            weight = jnp.where(tile_k == j, value, weight)
        return weight

    def apply(at_slots, indices):
        for slot in at_slots:
            weight = slot_weights(slot)
            for index in indices:
                real = shift_rows[index, 0] - h_rows[slot]
                imag = shift_rows[index, 1]
                inverse = 1.0 / (real * real + imag * imag)
                scale = jnp.where(tile_real, real * inverse, -imag * inverse)
                scales[index, slot] = scale
                rows_out[index, slot] = weight * scale
        side = jnp.concatenate([g_side[index] for index in indices], 0)
        for slot in at_slots:
            for c in range(pairs):
                product = times(side, right_ref[slot, c, 0], right_ref[slot, c, 1])
                for at, index in enumerate(indices):
                    q = g_shift[index] - product[at * orbitals : (at + 1) * orbitals]
                    d_real = scales[index, slot, c : c + 1, :]
                    d_imag = scales[index, slot, pairs + c : pairs + c + 1, :]
                    real, imag = q[:, :width], q[:, width:]
                    f_out[index, slot, c, 0] = eye_both - real * d_real + imag * d_imag
                    f_out[index, slot, c, 1] = -real * d_imag - imag * d_real

    prepare(place)
    unpack(0)
    beside.wait_recv()
    unpack(1)
    columns[0].wait_recv()
    prepare(others[0])
    apply([0, 1], [place, others[0]])
    for c in range(pairs):
        across[c].wait_recv()
        passes[c].start()
    unpack(2)
    apply([2], [place, others[0]])
    for copy in passes:
        copy.wait_recv()
    unpack(3)
    apply([3], [place, others[0]])
    for index in range(1, column - 1):
        columns[index].wait_recv()
        prepare(others[index])
    apply(range(slots), others[1:])
    for copy in columns + across + passes + [beside]:
        copy.wait_send()


def gather(hamiltonian, self_energy, guess_factor, weights, counts, column):
    k_local, orbitals, width = hamiltonian.shape
    pairs = k_local // 2
    return pl.pallas_call(
        gather_kernel,
        out_shape=(
            jax.ShapeDtypeStruct((column, 4, pairs, 2, orbitals, width), jnp.float32),
            jax.ShapeDtypeStruct((column, 4, k_local, width), jnp.float32),
            jax.ShapeDtypeStruct((column, 2, orbitals, width), jnp.float32),
            jax.ShapeDtypeStruct(counts.shape, jnp.int32),
        ),
        in_specs=[HBM] * 5,
        out_specs=(VMEM,) * 4,
        scratch_shapes=[
            pltpu.VMEM((k_local, orbitals, width), jnp.float32),
            pltpu.VMEM((4, pairs, orbitals, width), jnp.float32),
            pltpu.SMEM(weights.shape, jnp.int32),
            pltpu.VMEM((4, pairs, 2, width, 2 * width), jnp.bfloat16),
            pltpu.VMEM((column, orbitals, 3 * width), jnp.bfloat16),
            pltpu.VMEM((column, orbitals, 2 * width), jnp.float32),
            pltpu.VMEM((column, 2, k_local, width), jnp.float32),
            pltpu.VMEM((4, k_local, width), jnp.float32),
            pltpu.VMEM((column, 4, k_local, width), jnp.float32),
            pltpu.SemaphoreType.DMA((5,)),
            pltpu.SemaphoreType.DMA((2, 1)),
            pltpu.SemaphoreType.DMA((2, pairs)),
            pltpu.SemaphoreType.DMA((2, pairs)),
            pltpu.SemaphoreType.DMA((2, column)),
        ],
        compiler_params=pltpu.CompilerParams(collective_id=0, has_side_effects=True, vmem_limit_bytes=GRANT),
        name="gather",
    )(hamiltonian, self_energy, guess_factor, weights, counts)


class Tools:
    def __init__(self, orbitals, width):
        self.orbitals, self.width = orbitals, width
        shape = (orbitals, width)
        row = lax.broadcasted_iota(jnp.int32, shape, 0)
        lane = lax.broadcasted_iota(jnp.int32, shape, 1)
        self.left = lane < orbitals
        self.eye_both = (lax.rem(lane, orbitals) == row).astype(jnp.float32)
        self.eye_half = self.eye_both.astype(jnp.bfloat16)
        self.left_half = self.left.astype(jnp.float32).astype(jnp.bfloat16)
        self.right_half = (1.0 - self.left.astype(jnp.float32)).astype(jnp.bfloat16)
        self.left_mask = self.left_half > self.right_half

    def turn(self, value):
        return pltpu.roll(value, self.orbitals, 1)

    def columns(self, rows, index):
        slots, lines_each = rows.shape[1], rows.shape[2]
        lines = []
        for slot in range(slots):
            line = rows[index, slot]
            lines += [line, self.turn(line)]
        lines.append(jnp.zeros((self.width - 2 * lines_each * slots, self.width), jnp.float32))
        return jnp.transpose(jnp.concatenate(lines, 0))[: self.orbitals]

    def scaled(self, flat, pairs, p, real, imag):
        def column_of(at):
            return jnp.take_along_axis(flat, jnp.where(self.left, at, at + 2 * pairs), axis=1)

        first = (p // pairs) * 4 * pairs + p % pairs
        d_real, d_imag = column_of(first), column_of(first + pairs)
        return real * d_real - imag * d_imag, real * d_imag + imag * d_real

    def store_left(self, ref, index, at, high, low):
        span = slice(2 * at * self.width, 2 * (at + 1) * self.width)
        ref[index, : self.orbitals, span] = beside(high)
        ref[index, self.orbitals :, span] = beside(low)

    def store_right(self, ref, index, at, real, imag):
        lines = []
        for r, i in parts(self.eye_both + real, imag):
            r_turned, i_turned = self.turn(r), self.turn(i)
            lines.append(
                [
                    jnp.where(self.left_mask, r, i_turned),
                    jnp.where(self.left_mask, r_turned, i),
                    jnp.where(self.left_mask, -i, r_turned),
                    jnp.where(self.left_mask, -i_turned, r),
                ]
            )
        ref[index, 2 * at * self.width : 2 * (at + 1) * self.width, :] = grid_of(list(zip(*lines)))


def parts(real, imag):
    (real_high, real_low), (imag_high, imag_low) = halves(real), halves(imag)
    return (real_high, imag_high), (real_low, imag_low)


def beside(pair):
    return jnp.concatenate(pair, 1)


def newton_kernel(f_ref, rows, counts_ref, left_ref, right_ref, tail_ref, work, sides, counts):
    column, slots, pairs, _, orbitals, width = f_ref.shape
    total_pairs = slots * pairs
    kept = total_pairs - tail_ref.shape[1]
    parity = lax.rem(lax.axis_index("kgrp"), 2)
    branch = lax.rem(lax.axis_index("freq"), 2)
    steps = counts_ref[...]
    step_lane = lax.broadcasted_iota(jnp.int32, steps.shape, 1)
    for index in range(column):
        counts[index] = jnp.sum(jnp.where(step_lane == 2 * (2 * index + branch) + parity, steps, 0))
    tools = Tools(orbitals, width)
    eye_both = tools.eye_both

    def spread(real, imag):
        real_left, real_right = real * tools.left_half, real * tools.right_half
        imag_left, imag_right = imag * tools.left_half, imag * tools.right_half
        return grid_of(
            [
                [real_left, imag_left],
                [real_right, imag_right],
                [-imag_left, real_left],
                [-imag_right, real_right],
            ]
        )

    def multiply(highs, lows, right_high, right_low):
        count = len(highs) * orbitals
        high = jnp.concatenate(highs, 0)
        both = dot(jnp.concatenate([high] + lows, 0), spread(*right_high))
        return both[:count] + both[count:] + dot(high, spread(*right_low))

    def one_frequency(index, carry):
        count = counts[index]

        def load_f(p):
            return f_ref[index, p // pairs, p % pairs, 0], f_ref[index, p // pairs, p % pairs, 1]

        def squares(p):
            real, imag = load_f(p)
            high, low = parts(real, imag)
            sides[p, 0], sides[p, 1] = beside(high), beside(low)
            product = multiply([beside(high)], [beside(low)], high, low)
            work[p, 0] = product[:, :width]
            work[p, 1] = product[:, width:]

        def keep(p, values):
            for at, value in enumerate(values):
                if p >= kept:
                    tail_ref[index, p - kept, at] = value
                else:
                    work[p, 2 + at] = value

        def cubes(p):
            real, imag = load_f(p)
            square_real, square_imag = work[p, 0], work[p, 1]
            square_high, square_low = parts(square_real, square_imag)
            product = multiply(
                [sides[p, 0], beside(square_high)],
                [sides[p, 1], beside(square_low)],
                square_high,
                square_low,
            )
            keep(
                p,
                [
                    eye_both + real + square_real + product[:orbitals, :width],
                    imag + square_imag + product[:orbitals, width:],
                    product[orbitals:, :width],
                    product[orbitals:, width:],
                ],
            )

        def finish(flat, p, outer, inner):
            high, low = parts(*tools.scaled(flat, pairs, p, *outer))
            tools.store_left(left_ref, index, p, high, low)
            tools.store_right(right_ref, index, p, *inner)

        @pl.when(count == 1)
        def _():
            for p in range(total_pairs):
                slot, c = p // pairs, p % pairs
                real, imag = load_f(p)
                if p >= kept:
                    keep(p, [eye_both, jnp.zeros_like(eye_both), real, imag])
                    continue
                high, low = [
                    [tools.eye_half * line[at : at + 1, :] for at in (c, pairs + c)]
                    for line in halves(rows[index, slot])
                ]
                tools.store_left(left_ref, index, p, high, low)
                tools.store_right(right_ref, index, p, real, imag)

        @pl.when(count == 2)
        def _():
            flat = tools.columns(rows, index)
            for step in range(total_pairs + LAG):
                if step < total_pairs:
                    squares(step)
                if step >= LAG:
                    p = step - LAG
                    real, imag = load_f(p)
                    if p >= kept:
                        keep(p, [eye_both + real, imag, work[p, 0], work[p, 1]])
                    else:
                        finish(flat, p, (eye_both + real, imag), (work[p, 0], work[p, 1]))

        @pl.when(count > 2)
        def _():
            flat = tools.columns(rows, index)
            for step in range(total_pairs + 2 * LAG):
                if step < total_pairs:
                    squares(step)
                if LAG <= step < total_pairs + LAG:
                    cubes(step - LAG)
                if 2 * LAG <= step < kept + 2 * LAG:
                    p = step - 2 * LAG
                    finish(flat, p, (work[p, 2], work[p, 3]), (work[p, 4], work[p, 5]))

        return carry

    lax.fori_loop(0, column, one_frequency, 0)


def newton(f_values, rows, counts):
    column, slots, pairs, _, orbitals, width = f_values.shape
    depth = 2 * (slots * pairs - TAIL) * width
    return pl.pallas_call(
        newton_kernel,
        out_shape=(
            jax.ShapeDtypeStruct((column, 2 * orbitals, depth), jnp.bfloat16),
            jax.ShapeDtypeStruct((column, depth, 2 * width), jnp.bfloat16),
            jax.ShapeDtypeStruct((column, TAIL, 4, orbitals, width), jnp.float32),
        ),
        in_specs=[VMEM] * 3,
        out_specs=(VMEM,) * 3,
        scratch_shapes=[
            pltpu.VMEM((slots * pairs, 6, orbitals, width), jnp.float32),
            pltpu.VMEM((slots * pairs, 2, orbitals, 2 * width), jnp.bfloat16),
            pltpu.SMEM((column,), jnp.int32),
        ],
        compiler_params=pltpu.CompilerParams(vmem_limit_bytes=GRANT),
        name="newton",
    )(f_values, rows, counts)


def scatter_kernel(
    left_ref,
    right_ref,
    tail_ref,
    rows,
    sg_ref,
    weights_hbm,
    out_ref,
    weights,
    left_tail,
    right_tail,
    part,
    landed,
    load_sem,
    send,
    recv,
):
    freq_devs = lax.axis_size("freq")
    group_devs = lax.axis_size("kgrp")
    column, _, orbitals, width = sg_ref.shape
    tile = landed.shape[2]
    me = lax.axis_index("freq")
    group = lax.axis_index("kgrp")
    others = [(a, b) for a in range(freq_devs) for b in range(group_devs) if a + b > 0]
    barrier = pltpu.get_barrier_semaphore()

    def place(step):
        return lax.rem(me + step[0], freq_devs), lax.rem(group + step[1], group_devs)

    for freq_to in range(freq_devs):
        for group_to in range(group_devs):
            pl.semaphore_signal(barrier, inc=1, device_id=(freq_to, group_to), device_id_type=MESH)
    load = pltpu.make_async_copy(weights_hbm, weights, load_sem.at[0])
    load.start()

    def spread(index):
        freq_to, group_to = place(others[index])
        return pltpu.make_async_remote_copy(
            src_ref=part.at[pl.ds((freq_to * group_devs + group_to) * tile, tile)],
            dst_ref=landed.at[me, group],
            send_sem=send.at[index],
            recv_sem=recv.at[index],
            device_id=(freq_to, group_to),
            device_id_type=MESH,
        )

    wide_left = lax.broadcasted_iota(jnp.int32, (orbitals, width), 1) < orbitals
    tools = Tools(orbitals, width)
    pairs = rows.shape[2] // 2
    tail = tail_ref.shape[1]
    kept = rows.shape[1] * pairs - tail
    for index in range(column):
        flat = tools.columns(rows, index)
        for at in range(tail):
            high, low = parts(*tools.scaled(flat, pairs, kept + at, tail_ref[index, at, 0], tail_ref[index, at, 1]))
            tools.store_left(left_tail, index, at, high, low)
            tools.store_right(right_tail, index, at, tail_ref[index, at, 2], tail_ref[index, at, 3])
    step = 2 * width
    chunks = [(left_ref, right_ref, at * step) for at in range(kept)]
    chunks += [(left_tail, right_tail, at * step) for at in range(tail)]
    products = []
    for first in range(0, column, 2):
        sums = [None, None]
        for left_side, right_side, at in chunks:
            for offset in range(2):
                index = first + offset
                term = dot(left_side[index, :, at : at + step], right_side[index, at : at + step, :])
                sums[offset] = term if sums[offset] is None else sums[offset] + term
        products += sums
    for index in range(column):
        guess = sg_ref[index, 1]
        turned = pltpu.roll(guess, orbitals, 1)
        top = jnp.concatenate(halves(guess), 1)
        bottom = jnp.concatenate(halves(jnp.where(wide_left, -turned, turned)), 1)
        product = products[index]
        total = joined(product[:orbitals]) + product[orbitals:, :width]
        left_side = jnp.concatenate(halves(total), 1)
        green = joined(dot(left_side, jnp.concatenate([top, bottom, top, bottom], 0)))
        part[pl.ds(index, orbitals, stride=column), :] = green
    pl.semaphore_wait(barrier, len(others) + 1)

    def send_to(freq_to, group_to):
        ahead = lax.rem(freq_to - me + freq_devs, freq_devs)
        aside = lax.rem(group_to - group + group_devs, group_devs)
        slot = ahead * group_devs + aside - 1
        pltpu.make_async_remote_copy(
            src_ref=part.at[pl.ds((freq_to * group_devs + group_to) * tile, tile)],
            dst_ref=landed.at[me, group],
            send_sem=send.at[slot],
            recv_sem=recv.at[slot],
            device_id=(freq_to, group_to),
            device_id_type=MESH,
        ).start()

    for at in range(freq_devs - 1):
        freq_to = at + (at >= me).astype(jnp.int32)
        for group_to in range(group_devs):
            send_to(freq_to, jnp.int32(group_to))
    for at in range(group_devs - 1):
        send_to(me, at + (at >= group).astype(jnp.int32))
    landed[me, group] = part[pl.ds((me * group_devs + group) * tile, tile), :]
    load.wait()
    total = jnp.sum(weights[...].astype(jnp.float32), axis=0, keepdims=True)
    scale = 1.0 / jnp.broadcast_to(jnp.sum(total, axis=1, keepdims=True), (tile, width))
    for index in range(len(others)):
        spread(index).wait_recv()
    left = lax.broadcasted_iota(jnp.int32, (tile, width), 1) < orbitals
    freq_total = 4 * column
    for branch in range(2):
        for parity in range(2):
            total = None
            for place_at in range(column):
                for high in range(group_devs // 2):
                    term = landed[2 * place_at + branch, 2 * high + parity]
                    total = term if total is None else total + term
            total = total * scale
            swapped = pltpu.roll(total, tile // 2, 0)
            turned = pltpu.roll(total, orbitals, 1)
            turned_swapped = pltpu.roll(turned, tile // 2, 0)
            real = jnp.where(left, total, turned_swapped)
            imag = jnp.where(left, turned, swapped)
            first = 2 * branch + parity
            out_ref[pl.ds(first, column, stride=4), :] = real[:column]
            out_ref[pl.ds(freq_total + first, column, stride=4), :] = imag[:column]
    for index in range(len(others)):
        spread(index).wait_send()


def scatter(left, right, rest, rows, sigma_guess, weights, freq_devs, group_devs):
    column, _, orbitals, width = sigma_guess.shape
    tile = column * orbitals // (freq_devs * group_devs)
    peers = freq_devs * group_devs - 1
    return pl.pallas_call(
        scatter_kernel,
        out_shape=jax.ShapeDtypeStruct((8 * column, width), jnp.float32),
        in_specs=[VMEM] * 5 + [HBM],
        out_specs=VMEM,
        scratch_shapes=[
            pltpu.VMEM(weights.shape, jnp.int32),
            pltpu.VMEM((column, 2 * orbitals, 2 * TAIL * width), jnp.bfloat16),
            pltpu.VMEM((column, 2 * TAIL * width, 2 * width), jnp.bfloat16),
            pltpu.VMEM((column * orbitals, width), jnp.float32),
            pltpu.VMEM((freq_devs, group_devs, tile, width), jnp.float32),
            pltpu.SemaphoreType.DMA((1,)),
            pltpu.SemaphoreType.DMA((peers,)),
            pltpu.SemaphoreType.DMA((peers,)),
        ],
        compiler_params=pltpu.CompilerParams(collective_id=1, has_side_effects=True, vmem_limit_bytes=GRANT),
        name="scatter",
    )(left, right, rest, rows, sigma_guess, weights)


def per_device(hamiltonian, self_energy, guess_factor, weights, counts):
    k_local, orbitals, width = hamiltonian.shape
    per_freq = self_energy.shape[0]
    freq_devs = lax.axis_size("freq")
    group_devs = lax.axis_size("kgrp")
    freq_total = per_freq * freq_devs
    pair_block = orbitals * orbitals // (freq_devs * group_devs)
    column = freq_devs // 2
    direct = (
        width == 128
        and per_freq == 2
        and freq_devs % 2 == 0
        and group_devs % 2 == 0
        and pair_block == width
        and column == 4
        and k_local == 8
        and weights.shape[0] % width == 0
    )
    if direct:
        table = weights.reshape(-1, width)
        inputs = [
            pltpu.with_memory_space_constraint(value, pltpu.HBM)
            for value in (hamiltonian, self_energy, guess_factor, table, counts.reshape(1, -1))
        ]
        values, rows, sigma_guess, steps = gather(*inputs, column)
        left, right, rest = newton(values, rows, steps)
        return scatter(left, right, rest, rows, sigma_guess, inputs[3], freq_devs, group_devs).T
    sigma = lax.all_gather(self_energy, "freq", axis=0, tiled=True)
    guess = lax.all_gather(guess_factor, "freq", axis=0, tiled=True)
    current, factors = early_steps(counts, weights, hamiltonian, sigma, guess)
    terms = local_sum(factors, hamiltonian, sigma, current)
    terms = terms.reshape(freq_total, orbitals, 2, orbitals).transpose(1, 3, 2, 0)
    terms = terms.reshape(orbitals * orbitals, 2 * freq_total)
    result = lax.psum_scatter(terms, ("freq", "kgrp"), scatter_dimension=0, tiled=True)
    return result.reshape(pair_block, 2 * freq_total)


def solution(mesh):
    return jax.shard_map(
        per_device,
        mesh=mesh,
        in_specs=(
            P(("freq", "kgrp"), None, None),
            P("freq", None, None),
            P("freq", None, None),
            P(),
            P(),
        ),
        out_specs=P(("freq", "kgrp"), None),
        check_vma=False,
    )
```

```python
import functools
import math

import jax
import jax.numpy as jnp
from jax import lax
from jax.experimental import pallas as pl
from jax.experimental.pallas import tpu as pltpu
from jax.sharding import PartitionSpec as P

chem_potential = 0.2
MESH = pl.DeviceIdType.MESH
GRANT = 32 * 1024 * 1024
VMEM = pl.BlockSpec(memory_space=pltpu.VMEM)
SMEM = pl.BlockSpec(memory_space=pltpu.SMEM)
HBM = pl.BlockSpec(memory_space=pltpu.HBM)
LAG = 4
TAIL = 4


def split(value):
    high = value.astype(jnp.bfloat16).astype(jnp.float32)
    return high, value - high


def left_operand(value, half, left):
    high, low = split(value)
    turned_high, turned_low = split(pltpu.roll(value, half, 1))
    top = jnp.where(left, high, turned_low)
    bottom = jnp.where(left, turned_high, low)
    return jnp.concatenate([top, bottom], 0).astype(jnp.bfloat16)


def right_operand(value):
    high, low = split(value)
    row = jnp.concatenate([high, low], 1).astype(jnp.bfloat16)
    return jnp.concatenate([row, row], 0)


def fold(product, orbitals, sign):
    width = 2 * orbitals
    both = product[:, :width] + product[:, width:]
    return both[:orbitals] + sign * pltpu.roll(both[orbitals:], orbitals, 1)


def masks(shape):
    orbitals = shape[0]
    row = lax.broadcasted_iota(jnp.int32, shape, 0)
    lane = lax.broadcasted_iota(jnp.int32, shape, 1)
    left = lane < orbitals
    sign = jnp.where(left, -1.0, 1.0)
    eye_real = (lane == row).astype(jnp.float32)
    eye_imag = (lane == row + orbitals).astype(jnp.float32)
    return left, sign, eye_real, eye_imag


def shifted(freq, freq_total, eye_real, eye_imag, sigma):
    matsubara = (2 * freq + 1).astype(jnp.float32) * (math.pi / (2 * freq_total))
    return (chem_potential * eye_real + matsubara * eye_imag) - sigma


def steps_kernel(counts, weights, h_ref, sigma_ref, guess_ref, x_ref, factor_ref, m_left, h_diag):
    k_local, orbitals, width = h_ref.shape
    freq_total = sigma_ref.shape[0]
    shape = (orbitals, width)
    left, sign, eye_real, eye_imag = masks(shape)
    device = lax.axis_index("freq") * lax.axis_size("kgrp") + lax.axis_index("kgrp")

    def add_weight(index, total):
        return total + weights[index]

    weight_total = lax.fori_loop(
        0, weights.shape[0], add_weight, jnp.int32(0), unroll=8
    ).astype(jnp.float32)
    for k in range(k_local):
        weight = weights[device * k_local + k].astype(jnp.float32)
        factor_ref[k : k + 1, :] = jnp.full((1, width), weight) / weight_total

    def diagonal(value):
        real = jnp.sum(value * eye_real, axis=1, keepdims=True)
        imag = jnp.sum(value * eye_imag, axis=1, keepdims=True)
        return jnp.broadcast_to(real, shape), jnp.broadcast_to(imag, shape)

    for k in range(k_local):
        h_diag[0, k], h_diag[1, k] = diagonal(h_ref[k])

    def one_frequency(freq, carry):
        base = shifted(freq, freq_total, eye_real, eye_imag, sigma_ref[freq])
        base_real, base_imag = diagonal(base)
        guess = guess_ref[freq]
        turned = sign * pltpu.roll(guess, orbitals, 1)
        for k in range(k_local):
            real = base_real - h_diag[0, k]
            imag = base_imag - h_diag[1, k]
            inverse = 1.0 / (real * real + imag * imag)
            x_ref[freq, k] = (real * inverse) * guess - (imag * inverse) * turned

        @pl.when(counts[freq] > 1)
        def _():
            for k in range(k_local):
                m_left[k] = left_operand(base - h_ref[k], orbitals, left)

            def newton_step(sweep, inner):
                products = [
                    jnp.dot(
                        m_left[k],
                        right_operand(x_ref[freq, k]),
                        preferred_element_type=jnp.float32,
                    )
                    for k in range(k_local)
                ]
                products = [
                    jnp.dot(
                        left_operand(x_ref[freq, k], orbitals, left),
                        right_operand(eye_real - fold(products[k], orbitals, sign)),
                        preferred_element_type=jnp.float32,
                    )
                    for k in range(k_local)
                ]
                for k in range(k_local):
                    x_ref[freq, k] = x_ref[freq, k] + fold(products[k], orbitals, sign)
                return inner

            lax.fori_loop(0, counts[freq] - 1, newton_step, 0)

        return carry

    lax.fori_loop(0, freq_total, one_frequency, 0)


def early_steps(counts, weights, hamiltonian, sigma, guess):
    k_local, orbitals, width = hamiltonian.shape
    freq_total = sigma.shape[0]
    return pl.pallas_call(
        steps_kernel,
        out_shape=(
            jax.ShapeDtypeStruct((freq_total, k_local, orbitals, width), jnp.float32),
            jax.ShapeDtypeStruct((k_local, width), jnp.float32),
        ),
        in_specs=[SMEM, SMEM, VMEM, VMEM, VMEM],
        out_specs=(VMEM, VMEM),
        scratch_shapes=[
            pltpu.VMEM((k_local, width, width), jnp.bfloat16),
            pltpu.VMEM((2, k_local, orbitals, width), jnp.float32),
        ],
        compiler_params=pltpu.CompilerParams(vmem_limit_bytes=GRANT),
        name="early_steps",
    )(counts, weights, hamiltonian, sigma, guess)


def last_step(freq, freq_total, factor_ref, h_ref, sigma_ref, x_ref, last_left, last_right):
    k_local, orbitals, width = h_ref.shape
    left, sign, eye_real, eye_imag = masks((orbitals, width))
    base = shifted(freq, freq_total, eye_real, eye_imag, sigma_ref[freq])
    products = [
        jnp.dot(
            left_operand(base - h_ref[k], orbitals, left),
            right_operand(x_ref[freq, k]),
            preferred_element_type=jnp.float32,
        )
        for k in range(k_local)
    ]
    total = jnp.zeros((orbitals, width), jnp.float32)
    for k in range(k_local):
        weighted = x_ref[freq, k] * factor_ref[k : k + 1, :]
        last_left[:, k * width : (k + 1) * width] = left_operand(weighted, orbitals, left)
        total = total + weighted
    for k in range(k_local):
        missing = eye_real - fold(products[k], orbitals, sign)
        last_right[k * width : (k + 1) * width, :] = right_operand(missing)
    product = jnp.dot(last_left[...], last_right[...], preferred_element_type=jnp.float32)
    return total + fold(product, orbitals, sign)


def last_scratch(k_local, width):
    return [
        pltpu.VMEM((width, k_local * width), jnp.bfloat16),
        pltpu.VMEM((k_local * width, 2 * width), jnp.bfloat16),
    ]


def sum_kernel(factor_ref, h_ref, sigma_ref, x_ref, out_ref, last_left, last_right):
    freq_total = sigma_ref.shape[0]

    def one_frequency(freq, carry):
        out_ref[freq] = last_step(
            freq, freq_total, factor_ref, h_ref, sigma_ref, x_ref, last_left, last_right
        )
        return carry

    lax.fori_loop(0, freq_total, one_frequency, 0)


def local_sum(factors, hamiltonian, sigma, current):
    k_local, orbitals, width = hamiltonian.shape
    return pl.pallas_call(
        sum_kernel,
        out_shape=jax.ShapeDtypeStruct(sigma.shape, jnp.float32),
        in_specs=[VMEM] * 4,
        out_specs=VMEM,
        scratch_shapes=last_scratch(k_local, width),
        name="local_sum",
    )(factors, hamiltonian, sigma, current)


def halves(value):
    high = value.astype(jnp.bfloat16)
    return high, (value - high.astype(jnp.float32)).astype(jnp.bfloat16)


def joined(product):
    width = product.shape[1] // 2
    return product[:, :width] + product[:, width:]


def dot(left_side, right_side):
    return jnp.dot(left_side, right_side, preferred_element_type=jnp.float32)


def grid_of(blocks):
    return jnp.concatenate([jnp.concatenate(line, 1) for line in blocks], 0)


def gather_kernel(
    h_hbm,
    sigma_hbm,
    guess_hbm,
    weights_hbm,
    counts_hbm,
    f_out,
    rows_out,
    sg_out,
    counts_out,
    own_h,
    packed,
    weights,
    right_ref,
    g_side,
    g_shift,
    shift_rows,
    h_rows,
    scales,
    local,
    mate_sem,
    pair_sem,
    pass_sem,
    col_sem,
):
    column, slots, pairs, _, orbitals, width = f_out.shape
    k_local = 2 * pairs
    shape = (orbitals, width)
    freq_devs = 2 * column
    freq_total = 2 * freq_devs
    me = lax.axis_index("freq")
    group = lax.axis_index("kgrp")
    group_devs = lax.axis_size("kgrp")
    parity = lax.rem(group, 2)
    branch = lax.rem(me, 2)
    place = me // 2
    pair = me + 1 - 2 * branch
    mate = group + 1 - 2 * parity
    others = [place + 1 - 2 * lax.rem(place, 2), lax.rem(place + 2, column), column - 1 - place]
    barrier = pltpu.get_barrier_semaphore()
    for other in others:
        pl.semaphore_signal(barrier, inc=1, device_id=(2 * other + branch, group), device_id_type=MESH)
    pl.semaphore_signal(barrier, inc=1, device_id=(pair, group), device_id_type=MESH)
    pl.semaphore_signal(barrier, inc=1, device_id=(me, mate), device_id_type=MESH)
    loads = [
        pltpu.make_async_copy(h_hbm, own_h, local.at[0]),
        pltpu.make_async_copy(sigma_hbm.at[parity], sg_out.at[place, 0], local.at[1]),
        pltpu.make_async_copy(guess_hbm.at[parity], sg_out.at[place, 1], local.at[2]),
        pltpu.make_async_copy(weights_hbm, weights, local.at[3]),
        pltpu.make_async_copy(counts_hbm, counts_out, local.at[4]),
    ]
    for load in loads:
        load.start()

    def remote(src, dst, sems, slot, freq_to, group_to):
        return pltpu.make_async_remote_copy(
            src_ref=src,
            dst_ref=dst,
            send_sem=sems.at[0, slot],
            recv_sem=sems.at[1, slot],
            device_id=(freq_to, group_to),
            device_id_type=MESH,
        )

    own = sg_out.at[place]
    columns = [
        remote(own, own, col_sem, index, 2 * others[index] + branch, group) for index in range(column - 1)
    ]
    across = [remote(packed.at[0, c], packed.at[2, c], pair_sem, c, pair, group) for c in range(pairs)]
    passes = [remote(packed.at[2, c], packed.at[3, c], pass_sem, c, me, mate) for c in range(pairs)]
    beside = remote(packed.at[0], packed.at[1], mate_sem, 0, me, mate)

    row = lax.broadcasted_iota(jnp.int32, shape, 0)
    lane = lax.broadcasted_iota(jnp.int32, shape, 1)
    left = lane < orbitals
    within = jnp.where(left, lane, lane - orbitals)
    upper = within >= row
    above = within > row
    eye_both = (within == row).astype(jnp.float32)

    def turn(value):
        return pltpu.roll(value, orbitals, 1)

    def planes(slot, c, real, imag):
        diagonal = jnp.sum(eye_both * real, axis=0, keepdims=True)
        h_rows[slot, c : c + 1, :] = diagonal
        h_rows[slot, pairs + c : pairs + c + 1, :] = diagonal
        for part, (r, i) in enumerate(zip(halves(real), halves(imag))):
            right_ref[slot, c, part] = grid_of([[r, i], [-i, r]])

    loads[0].wait()
    for c in range(pairs):
        one, two = own_h[2 * c], own_h[2 * c + 1]
        real = jnp.where(left, one, turn(two))
        imag = jnp.where(left, turn(one), two)
        packed[0, c] = jnp.where(upper, real, imag)
    loads[1].wait()
    loads[2].wait()
    pl.semaphore_wait(barrier, column + 1)
    for copy in columns + across + [beside]:
        copy.start()
    loads[3].wait()
    loads[4].wait()

    def times(guess_side, right_high, right_low):
        return dot(guess_side, jnp.concatenate([right_high, right_high, right_low], 0))

    def prepare(index):
        frequency = 2 * (2 * index + branch) + parity
        matsubara = (2 * frequency + 1).astype(jnp.float32) * (math.pi / (2 * freq_total))
        sigma = sg_out[index, 0]
        swapped = turn(sigma)
        real = chem_potential * eye_both - jnp.where(left, sigma, swapped)
        imag = matsubara * eye_both - jnp.where(left, swapped, sigma)
        high, low = halves(sg_out[index, 1])
        guess_side = jnp.concatenate([high, low, high], 1)
        g_side[index] = guess_side
        shift_rows[index, 0] = jnp.broadcast_to(jnp.sum(eye_both * real, axis=0, keepdims=True), tile)
        shift_rows[index, 1] = jnp.broadcast_to(jnp.sum(eye_both * imag, axis=0, keepdims=True), tile)
        (real_high, real_low), (imag_high, imag_low) = halves(real), halves(imag)
        product = times(
            guess_side,
            grid_of([[real_high, imag_high], [-imag_high, real_high]]),
            grid_of([[real_low, imag_low], [-imag_low, real_low]]),
        )
        g_shift[index] = product

    def unpack(slot):
        for c in range(pairs):
            value = packed[slot, c]
            flipped = jnp.transpose(value)
            other = jnp.concatenate([flipped[:orbitals], flipped[orbitals:]], 1)
            real = jnp.where(upper, value, other)
            imag = jnp.where(above, -other, jnp.where(upper, 0.0, value))
            planes(slot, c, real, imag)

    tile = (2 * pairs, width)
    tile_row = lax.broadcasted_iota(jnp.int32, tile, 0)
    tile_left = lax.broadcasted_iota(jnp.int32, tile, 1) < orbitals
    tile_real = tile_row < pairs
    tile_k = 2 * jnp.where(tile_real, tile_row, tile_row - pairs) + jnp.where(tile_left, 0, 1)

    def slot_weights(slot):
        owner_freq = me + (slot // 2) * (1 - 2 * branch)
        owner_group = group + (slot % 2) * (1 - 2 * parity)
        k_first = (owner_freq * group_devs + owner_group) * k_local
        first_row, first_column = lax.div(k_first, width), lax.rem(k_first, width)
        weight = jnp.zeros(tile, jnp.float32)
        for j in range(k_local):
            value = weights[first_row, first_column + j].astype(jnp.float32)
            weight = jnp.where(tile_k == j, value, weight)
        return weight

    def apply(at_slots, indices):
        for slot in at_slots:
            weight = slot_weights(slot)
            for index in indices:
                real = shift_rows[index, 0] - h_rows[slot]
                imag = shift_rows[index, 1]
                inverse = 1.0 / (real * real + imag * imag)
                scale = jnp.where(tile_real, real * inverse, -imag * inverse)
                scales[index, slot] = scale
                rows_out[index, slot] = weight * scale
        side = jnp.concatenate([g_side[index] for index in indices], 0)
        for slot in at_slots:
            for c in range(pairs):
                product = times(side, right_ref[slot, c, 0], right_ref[slot, c, 1])
                for at, index in enumerate(indices):
                    q = g_shift[index] - product[at * orbitals : (at + 1) * orbitals]
                    d_real = scales[index, slot, c : c + 1, :]
                    d_imag = scales[index, slot, pairs + c : pairs + c + 1, :]
                    real, imag = q[:, :width], q[:, width:]
                    f_out[index, slot, c, 0] = eye_both - real * d_real + imag * d_imag
                    f_out[index, slot, c, 1] = -real * d_imag - imag * d_real

    prepare(place)
    unpack(0)
    beside.wait_recv()
    unpack(1)
    columns[0].wait_recv()
    prepare(others[0])
    apply([0, 1], [place, others[0]])
    for c in range(pairs):
        across[c].wait_recv()
        passes[c].start()
    unpack(2)
    apply([2], [place, others[0]])
    for copy in passes:
        copy.wait_recv()
    unpack(3)
    apply([3], [place, others[0]])
    for index in range(1, column - 1):
        columns[index].wait_recv()
        prepare(others[index])
    apply(range(slots), others[1:])
    for copy in columns + across + passes + [beside]:
        copy.wait_send()


def gather(hamiltonian, self_energy, guess_factor, weights, counts, column):
    k_local, orbitals, width = hamiltonian.shape
    pairs = k_local // 2
    return pl.pallas_call(
        gather_kernel,
        out_shape=(
            jax.ShapeDtypeStruct((column, 4, pairs, 2, orbitals, width), jnp.float32),
            jax.ShapeDtypeStruct((column, 4, k_local, width), jnp.float32),
            jax.ShapeDtypeStruct((column, 2, orbitals, width), jnp.float32),
            jax.ShapeDtypeStruct(counts.shape, jnp.int32),
        ),
        in_specs=[HBM] * 5,
        out_specs=(VMEM,) * 4,
        scratch_shapes=[
            pltpu.VMEM((k_local, orbitals, width), jnp.float32),
            pltpu.VMEM((4, pairs, orbitals, width), jnp.float32),
            pltpu.SMEM(weights.shape, jnp.int32),
            pltpu.VMEM((4, pairs, 2, width, 2 * width), jnp.bfloat16),
            pltpu.VMEM((column, orbitals, 3 * width), jnp.bfloat16),
            pltpu.VMEM((column, orbitals, 2 * width), jnp.float32),
            pltpu.VMEM((column, 2, k_local, width), jnp.float32),
            pltpu.VMEM((4, k_local, width), jnp.float32),
            pltpu.VMEM((column, 4, k_local, width), jnp.float32),
            pltpu.SemaphoreType.DMA((5,)),
            pltpu.SemaphoreType.DMA((2, 1)),
            pltpu.SemaphoreType.DMA((2, pairs)),
            pltpu.SemaphoreType.DMA((2, pairs)),
            pltpu.SemaphoreType.DMA((2, column)),
        ],
        compiler_params=pltpu.CompilerParams(collective_id=0, has_side_effects=True, vmem_limit_bytes=GRANT),
        name="gather",
    )(hamiltonian, self_energy, guess_factor, weights, counts)


class Tools:
    def __init__(self, orbitals, width):
        self.orbitals, self.width = orbitals, width
        shape = (orbitals, width)
        row = lax.broadcasted_iota(jnp.int32, shape, 0)
        lane = lax.broadcasted_iota(jnp.int32, shape, 1)
        self.left = lane < orbitals
        self.eye_both = (lax.rem(lane, orbitals) == row).astype(jnp.float32)
        self.eye_half = self.eye_both.astype(jnp.bfloat16)
        self.left_half = self.left.astype(jnp.float32).astype(jnp.bfloat16)
        self.right_half = (1.0 - self.left.astype(jnp.float32)).astype(jnp.bfloat16)
        self.left_mask = self.left_half > self.right_half

    def turn(self, value):
        return pltpu.roll(value, self.orbitals, 1)

    def columns(self, rows, index):
        slots, lines_each = rows.shape[1], rows.shape[2]
        lines = []
        for slot in range(slots):
            line = rows[index, slot]
            lines += [line, self.turn(line)]
        lines.append(jnp.zeros((self.width - 2 * lines_each * slots, self.width), jnp.float32))
        return jnp.transpose(jnp.concatenate(lines, 0))[: self.orbitals]

    def scaled(self, flat, pairs, p, real, imag):
        def column_of(at):
            return jnp.take_along_axis(flat, jnp.where(self.left, at, at + 2 * pairs), axis=1)

        first = (p // pairs) * 4 * pairs + p % pairs
        d_real, d_imag = column_of(first), column_of(first + pairs)
        return real * d_real - imag * d_imag, real * d_imag + imag * d_real

    def store_left(self, ref, index, at, high, low):
        span = slice(2 * at * self.width, 2 * (at + 1) * self.width)
        ref[index, : self.orbitals, span] = beside(high)
        ref[index, self.orbitals :, span] = beside(low)

    def store_right(self, ref, index, at, real, imag):
        lines = []
        for r, i in parts(self.eye_both + real, imag):
            r_turned, i_turned = self.turn(r), self.turn(i)
            lines.append(
                [
                    jnp.where(self.left_mask, r, i_turned),
                    jnp.where(self.left_mask, r_turned, i),
                    jnp.where(self.left_mask, -i, r_turned),
                    jnp.where(self.left_mask, -i_turned, r),
                ]
            )
        ref[index, 2 * at * self.width : 2 * (at + 1) * self.width, :] = grid_of(list(zip(*lines)))


def parts(real, imag):
    (real_high, real_low), (imag_high, imag_low) = halves(real), halves(imag)
    return (real_high, imag_high), (real_low, imag_low)


def beside(pair):
    return jnp.concatenate(pair, 1)


def newton_kernel(f_ref, rows, counts_ref, left_ref, right_ref, tail_ref, work, sides, counts):
    column, slots, pairs, _, orbitals, width = f_ref.shape
    total_pairs = slots * pairs
    kept = total_pairs - tail_ref.shape[1]
    parity = lax.rem(lax.axis_index("kgrp"), 2)
    branch = lax.rem(lax.axis_index("freq"), 2)
    steps = counts_ref[...]
    step_lane = lax.broadcasted_iota(jnp.int32, steps.shape, 1)
    for index in range(column):
        counts[index] = jnp.sum(jnp.where(step_lane == 2 * (2 * index + branch) + parity, steps, 0))
    tools = Tools(orbitals, width)
    eye_both = tools.eye_both

    def spread(real, imag):
        real_left, real_right = real * tools.left_half, real * tools.right_half
        imag_left, imag_right = imag * tools.left_half, imag * tools.right_half
        return grid_of(
            [
                [real_left, imag_left],
                [real_right, imag_right],
                [-imag_left, real_left],
                [-imag_right, real_right],
            ]
        )

    def multiply(highs, lows, right_high, right_low):
        count = len(highs) * orbitals
        high = jnp.concatenate(highs, 0)
        both = dot(jnp.concatenate([high] + lows, 0), spread(*right_high))
        return both[:count] + both[count:] + dot(high, spread(*right_low))

    def one_frequency(index, carry):
        count = counts[index]

        def load_f(p):
            return f_ref[index, p // pairs, p % pairs, 0], f_ref[index, p // pairs, p % pairs, 1]

        def squares(p):
            real, imag = load_f(p)
            high, low = parts(real, imag)
            sides[p, 0], sides[p, 1] = beside(high), beside(low)
            product = multiply([beside(high)], [beside(low)], high, low)
            work[p, 0] = product[:, :width]
            work[p, 1] = product[:, width:]

        def keep(p, values):
            for at, value in enumerate(values):
                if p >= kept:
                    tail_ref[index, p - kept, at] = value
                else:
                    work[p, 2 + at] = value

        def cubes(p):
            real, imag = load_f(p)
            square_real, square_imag = work[p, 0], work[p, 1]
            square_high, square_low = parts(square_real, square_imag)
            product = multiply(
                [sides[p, 0], beside(square_high)],
                [sides[p, 1], beside(square_low)],
                square_high,
                square_low,
            )
            keep(
                p,
                [
                    eye_both + real + square_real + product[:orbitals, :width],
                    imag + square_imag + product[:orbitals, width:],
                    product[orbitals:, :width],
                    product[orbitals:, width:],
                ],
            )

        def finish(flat, p, outer, inner):
            high, low = parts(*tools.scaled(flat, pairs, p, *outer))
            tools.store_left(left_ref, index, p, high, low)
            tools.store_right(right_ref, index, p, *inner)

        @pl.when(count == 1)
        def _():
            for p in range(total_pairs):
                slot, c = p // pairs, p % pairs
                real, imag = load_f(p)
                if p >= kept:
                    keep(p, [eye_both, jnp.zeros_like(eye_both), real, imag])
                    continue
                high, low = [
                    [tools.eye_half * line[at : at + 1, :] for at in (c, pairs + c)]
                    for line in halves(rows[index, slot])
                ]
                tools.store_left(left_ref, index, p, high, low)
                tools.store_right(right_ref, index, p, real, imag)

        @pl.when(count == 2)
        def _():
            flat = tools.columns(rows, index)
            for step in range(total_pairs + LAG):
                if step < total_pairs:
                    squares(step)
                if step >= LAG:
                    p = step - LAG
                    real, imag = load_f(p)
                    if p >= kept:
                        keep(p, [eye_both + real, imag, work[p, 0], work[p, 1]])
                    else:
                        finish(flat, p, (eye_both + real, imag), (work[p, 0], work[p, 1]))

        @pl.when(count > 2)
        def _():
            flat = tools.columns(rows, index)
            for step in range(total_pairs + 2 * LAG):
                if step < total_pairs:
                    squares(step)
                if LAG <= step < total_pairs + LAG:
                    cubes(step - LAG)
                if 2 * LAG <= step < kept + 2 * LAG:
                    p = step - 2 * LAG
                    finish(flat, p, (work[p, 2], work[p, 3]), (work[p, 4], work[p, 5]))

        return carry

    lax.fori_loop(0, column, one_frequency, 0)


def newton(f_values, rows, counts):
    column, slots, pairs, _, orbitals, width = f_values.shape
    depth = 2 * (slots * pairs - TAIL) * width
    return pl.pallas_call(
        newton_kernel,
        out_shape=(
            jax.ShapeDtypeStruct((column, 2 * orbitals, depth), jnp.bfloat16),
            jax.ShapeDtypeStruct((column, depth, 2 * width), jnp.bfloat16),
            jax.ShapeDtypeStruct((column, TAIL, 4, orbitals, width), jnp.float32),
        ),
        in_specs=[VMEM] * 3,
        out_specs=(VMEM,) * 3,
        scratch_shapes=[
            pltpu.VMEM((slots * pairs, 6, orbitals, width), jnp.float32),
            pltpu.VMEM((slots * pairs, 2, orbitals, 2 * width), jnp.bfloat16),
            pltpu.SMEM((column,), jnp.int32),
        ],
        compiler_params=pltpu.CompilerParams(vmem_limit_bytes=GRANT),
        name="newton",
    )(f_values, rows, counts)


def scatter_kernel(
    left_ref,
    right_ref,
    tail_ref,
    rows,
    sg_ref,
    weights_hbm,
    out_ref,
    weights,
    left_tail,
    right_tail,
    part,
    landed,
    load_sem,
    send,
    recv,
):
    freq_devs = lax.axis_size("freq")
    group_devs = lax.axis_size("kgrp")
    column, _, orbitals, width = sg_ref.shape
    tile = landed.shape[2]
    me = lax.axis_index("freq")
    group = lax.axis_index("kgrp")
    others = [(a, b) for a in range(freq_devs) for b in range(group_devs) if a + b > 0]
    barrier = pltpu.get_barrier_semaphore()

    def place(step):
        return lax.rem(me + step[0], freq_devs), lax.rem(group + step[1], group_devs)

    for freq_to in range(freq_devs):
        for group_to in range(group_devs):
            pl.semaphore_signal(barrier, inc=1, device_id=(freq_to, group_to), device_id_type=MESH)
    load = pltpu.make_async_copy(weights_hbm, weights, load_sem.at[0])
    load.start()

    def spread(index):
        freq_to, group_to = place(others[index])
        return pltpu.make_async_remote_copy(
            src_ref=part.at[pl.ds((freq_to * group_devs + group_to) * tile, tile)],
            dst_ref=landed.at[me, group],
            send_sem=send.at[index],
            recv_sem=recv.at[index],
            device_id=(freq_to, group_to),
            device_id_type=MESH,
        )

    wide_left = lax.broadcasted_iota(jnp.int32, (orbitals, width), 1) < orbitals
    tools = Tools(orbitals, width)
    pairs = rows.shape[2] // 2
    tail = tail_ref.shape[1]
    kept = rows.shape[1] * pairs - tail
    for index in range(column):
        flat = tools.columns(rows, index)
        for at in range(tail):
            high, low = parts(*tools.scaled(flat, pairs, kept + at, tail_ref[index, at, 0], tail_ref[index, at, 1]))
            tools.store_left(left_tail, index, at, high, low)
            tools.store_right(right_tail, index, at, tail_ref[index, at, 2], tail_ref[index, at, 3])
    step = 2 * width
    chunks = [(left_ref, right_ref, at * step) for at in range(kept)]
    chunks += [(left_tail, right_tail, at * step) for at in range(tail)]
    products = [None] * column

    def add(first, some):
        for left_side, right_side, at in some:
            for index in range(column):
                term = dot(left_side[index, :, at : at + step], right_side[index, at : at + step, :])
                products[index] = term if products[index] is None else products[index] + term

    for first in range(0, column, column):
        add(first, chunks[:kept])
    for first in range(0, column, column):
        add(first, chunks[kept:])
    for index in range(column):
        guess = sg_ref[index, 1]
        turned = pltpu.roll(guess, orbitals, 1)
        top = jnp.concatenate(halves(guess), 1)
        bottom = jnp.concatenate(halves(jnp.where(wide_left, -turned, turned)), 1)
        product = products[index]
        total = joined(product[:orbitals]) + product[orbitals:, :width]
        left_side = jnp.concatenate(halves(total), 1)
        green = joined(dot(left_side, jnp.concatenate([top, bottom, top, bottom], 0)))
        part[pl.ds(index, orbitals, stride=column), :] = green
    pl.semaphore_wait(barrier, len(others) + 1)

    def send_to(freq_to, group_to):
        ahead = lax.rem(freq_to - me + freq_devs, freq_devs)
        aside = lax.rem(group_to - group + group_devs, group_devs)
        slot = ahead * group_devs + aside - 1
        pltpu.make_async_remote_copy(
            src_ref=part.at[pl.ds((freq_to * group_devs + group_to) * tile, tile)],
            dst_ref=landed.at[me, group],
            send_sem=send.at[slot],
            recv_sem=recv.at[slot],
            device_id=(freq_to, group_to),
            device_id_type=MESH,
        ).start()

    for at in range(freq_devs - 1):
        freq_to = at + (at >= me).astype(jnp.int32)
        for group_to in range(group_devs):
            send_to(freq_to, jnp.int32(group_to))
    for at in range(group_devs - 1):
        send_to(me, at + (at >= group).astype(jnp.int32))
    landed[me, group] = part[pl.ds((me * group_devs + group) * tile, tile), :]
    load.wait()
    total = jnp.sum(weights[...].astype(jnp.float32), axis=0, keepdims=True)
    scale = 1.0 / jnp.broadcast_to(jnp.sum(total, axis=1, keepdims=True), (tile, width))
    for index in range(len(others)):
        spread(index).wait_recv()
    left = lax.broadcasted_iota(jnp.int32, (tile, width), 1) < orbitals
    freq_total = 4 * column
    for branch in range(2):
        for parity in range(2):
            total = None
            for place_at in range(column):
                for high in range(group_devs // 2):
                    term = landed[2 * place_at + branch, 2 * high + parity]
                    total = term if total is None else total + term
            total = total * scale
            swapped = pltpu.roll(total, tile // 2, 0)
            turned = pltpu.roll(total, orbitals, 1)
            turned_swapped = pltpu.roll(turned, tile // 2, 0)
            real = jnp.where(left, total, turned_swapped)
            imag = jnp.where(left, turned, swapped)
            first = 2 * branch + parity
            out_ref[pl.ds(first, column, stride=4), :] = real[:column]
            out_ref[pl.ds(freq_total + first, column, stride=4), :] = imag[:column]
    for index in range(len(others)):
        spread(index).wait_send()


def scatter(left, right, rest, rows, sigma_guess, weights, freq_devs, group_devs):
    column, _, orbitals, width = sigma_guess.shape
    tile = column * orbitals // (freq_devs * group_devs)
    peers = freq_devs * group_devs - 1
    return pl.pallas_call(
        scatter_kernel,
        out_shape=jax.ShapeDtypeStruct((8 * column, width), jnp.float32),
        in_specs=[VMEM] * 5 + [HBM],
        out_specs=VMEM,
        scratch_shapes=[
            pltpu.VMEM(weights.shape, jnp.int32),
            pltpu.VMEM((column, 2 * orbitals, 2 * TAIL * width), jnp.bfloat16),
            pltpu.VMEM((column, 2 * TAIL * width, 2 * width), jnp.bfloat16),
            pltpu.VMEM((column * orbitals, width), jnp.float32),
            pltpu.VMEM((freq_devs, group_devs, tile, width), jnp.float32),
            pltpu.SemaphoreType.DMA((1,)),
            pltpu.SemaphoreType.DMA((peers,)),
            pltpu.SemaphoreType.DMA((peers,)),
        ],
        compiler_params=pltpu.CompilerParams(collective_id=1, has_side_effects=True, vmem_limit_bytes=GRANT),
        name="scatter",
    )(left, right, rest, rows, sigma_guess, weights)


def per_device(hamiltonian, self_energy, guess_factor, weights, counts):
    k_local, orbitals, width = hamiltonian.shape
    per_freq = self_energy.shape[0]
    freq_devs = lax.axis_size("freq")
    group_devs = lax.axis_size("kgrp")
    freq_total = per_freq * freq_devs
    pair_block = orbitals * orbitals // (freq_devs * group_devs)
    column = freq_devs // 2
    direct = (
        width == 128
        and per_freq == 2
        and freq_devs % 2 == 0
        and group_devs % 2 == 0
        and pair_block == width
        and column == 4
        and k_local == 8
        and weights.shape[0] % width == 0
    )
    if direct:
        table = weights.reshape(-1, width)
        inputs = [
            pltpu.with_memory_space_constraint(value, pltpu.HBM)
            for value in (hamiltonian, self_energy, guess_factor, table, counts.reshape(1, -1))
        ]
        values, rows, sigma_guess, steps = gather(*inputs, column)
        left, right, rest = newton(values, rows, steps)
        return scatter(left, right, rest, rows, sigma_guess, inputs[3], freq_devs, group_devs).T
    sigma = lax.all_gather(self_energy, "freq", axis=0, tiled=True)
    guess = lax.all_gather(guess_factor, "freq", axis=0, tiled=True)
    current, factors = early_steps(counts, weights, hamiltonian, sigma, guess)
    terms = local_sum(factors, hamiltonian, sigma, current)
    terms = terms.reshape(freq_total, orbitals, 2, orbitals).transpose(1, 3, 2, 0)
    terms = terms.reshape(orbitals * orbitals, 2 * freq_total)
    result = lax.psum_scatter(terms, ("freq", "kgrp"), scatter_dimension=0, tiled=True)
    return result.reshape(pair_block, 2 * freq_total)


def solution(mesh):
    return jax.shard_map(
        per_device,
        mesh=mesh,
        in_specs=(
            P(("freq", "kgrp"), None, None),
            P("freq", None, None),
            P("freq", None, None),
            P(),
            P(),
        ),
        out_specs=P(("freq", "kgrp"), None),
        check_vma=False,
    )
```
